1024 devices in a mesh: node: 32 (over z, core), local: 32 (over y, x).
Axes of the slice: x: 4, y: 8, z: 16, core: 2. Of those that a mesh axis runs over, the one named last changes fastest.
Arguments:
- tokens: bfloat16 [32, 32, 7168], P('local', 'node'), may hold values from -6 to 6
- node_ids: int32 [32, 32, 4], P('local', 'node'), may hold values from 0 to 15, all different within a row; in each aligned block of 32 rows (0 to 31, 32 to 63, ..., all dimensions but the last counted through in order) at most 9 rows name the same one
- gates: bfloat16 [32, 32, 8], P('local', 'node'), may hold values from 0.19921875 to 2
- w_in: bfloat16 [1024, 3584, 256], P(('node', 'local')), may hold values from -0.0625 to 0.0625
- w_out: bfloat16 [32, 2048, 7168], P('node', 'local'), may hold values from -0.125 to 0.125
Outputs:
- mixed: bfloat16 [32, 32, 7168], P('local', 'node')
- balance: float32 [32], P('node')
The draws below stay inside these ranges and needn't reach their ends.
Inputs may be any that keep to these rules, and one draw needn't show every extreme that they name: `node_ids`: each token names 4 different nodes. Among the 32 tokens of one index along the first dimension, no node is named by more than 9 tokens, and in every draw, for some index, some node is named by exactly 9 of them.
All inputs are finite; a program needn't handle non-finite values.
Results may differ from the reference program's by a relative error of at most 0.017.
Values may be sent and summed in bfloat16 or wider, within the bound.
No kernel may reach another device: no remote copies, remote signals or barrier semaphores. Data moves between devices by JAX's collectives and lax.ppermute only.
A program may use at most 64 MiB of HBM per device.

```python
import math
import jax
import jax.numpy as jnp
import numpy as np
from jax import lax

D = 7168
FF = 2048
NODE_TOP = 4
TOK_DEV = 1
TOP = 8
GROUPS = 16
RECV = 9
FF_DEV = 128
N_NODE = 32
N_LOCAL = 32


def shard_levels(key, shape, pieces, smallest, top_value):
    factor_of, own = 1.0, jax.random.fold_in(key, 6)
    for dim, blocks in pieces:
        steps = jnp.exp(jax.random.uniform(jax.random.fold_in(own, dim), (blocks,), jnp.float32, smallest / len(pieces), top_value / len(pieces)))
        factor_of = factor_of * jnp.repeat(steps, shape[dim] // blocks).reshape([-1 if axis == dim else 1 for axis in range(len(shape))])
    return factor_of


def routed_block(stream_key, own, number, rows, number_of, top, limit, lean):
    order = jax.random.permutation(stream_key, number_of)
    heavy_load, usual = shares(number_of, rows * top, limit, lean, True), shares(number_of, rows * top, limit, lean, False)
    places = jnp.arange(number_of)

    def named(lengths, rotation):
        used = int((lengths > 0).sum())
        fixed = max(1, used // 4)
        shifted = fixed + (places - fixed + rotation * (used - fixed)) % max(1, number_of - fixed)
        return jnp.zeros((number_of,), jnp.int32).at[order[jnp.where(places < fixed, places, shifted)]].set(jnp.asarray(lengths, jnp.int32))

    lengths = jnp.where(number % 4 == 0, named(heavy_load, number // 4), named(usual, number - number // 4 - 1))
    mixed = jax.random.permutation(jax.random.fold_in(own, 3), number_of)
    donor, taker = mixed[0:number_of // 2 * 2:2], mixed[1:number_of // 2 * 2:2]
    room = jnp.minimum(lengths[donor] - 1, limit - lengths[taker]) // 2
    room = jnp.where((donor == order[0]) | (taker == order[0]) | (lengths[taker] == 0), 0, jnp.maximum(room, 0))
    shifted = jax.random.randint(jax.random.fold_in(own, 4), (number_of // 2,), 0, 1 << 20) % (room + 1)
    lengths = lengths.at[donor].add(-shifted).at[taker].add(shifted)
    members = jnp.searchsorted(jnp.cumsum(lengths), jnp.arange(rows * top), side="right").astype(jnp.int32)
    grid = members.reshape(top, rows).T
    grid = grid[jax.random.permutation(jax.random.fold_in(own, 1), rows)]
    rotation = jax.random.randint(jax.random.fold_in(own, 2), (rows, 1), 0, top)
    return jnp.take_along_axis(grid, (jnp.arange(top)[None, :] + rotation) % top, axis=1)


def shares(number_of, total, reach, lean, full):
    loads = [(1 << 20) // math.isqrt(grade ** lean) + 1 for grade in range(1, number_of + 1)]
    largest = reach if full else min(reach, max(-(-total // number_of), total * loads[0] // sum(loads)))
    least = 1 if total - largest >= number_of - 1 else 0
    given, rest = [largest] + [least] * (number_of - 1), total - largest - least * (number_of - 1)
    while rest > 0:
        free = [i for i in range(1, number_of) if given[i] < largest] or [i for i in range(1, number_of) if given[i] < reach]
        mass, left = sum([loads[i] for i in free]), rest
        for i in free:
            addition = min(reach - given[i], max(1, left * loads[i] // mass), rest)
            given[i] = given[i] + addition
            rest = rest - addition
    return np.array(given)


def gaussian(stream_key, shape, scale, reach, cuts=(), held_as=jnp.bfloat16):
    values = scale * jax.random.normal(stream_key, shape, jnp.float32)
    if cuts:
        values = values * shard_levels(stream_key, shape, cuts, -0.22, 0.18)
    return jnp.clip(values, -reach, reach).astype(held_as)


def setup_inputs(seed: int = 0) -> dict:
    key_of = jax.random.split(jax.random.key(seed), 6)
    tokens = gaussian(key_of[0], (N_LOCAL, N_NODE * TOK_DEV, D), 1.0, 6.0, ((0, 32), (1, 32)))
    node_ids_keys = jax.random.split(jax.random.fold_in(key_of[1], 1), N_LOCAL * (N_NODE * TOK_DEV) // (N_NODE * TOK_DEV))
    node_ids_turns = jax.random.permutation(jax.random.fold_in(key_of[1], 3), N_LOCAL * (N_NODE * TOK_DEV) // (N_NODE * TOK_DEV))
    node_ids = jax.vmap(lambda own, number: routed_block(jax.random.fold_in(key_of[1], 2), own, number, N_NODE * TOK_DEV, GROUPS, NODE_TOP, RECV, 2))(node_ids_keys, node_ids_turns).reshape((N_LOCAL, N_NODE * TOK_DEV, NODE_TOP))
    gates = jnp.clip(jnp.exp(math.log(2.0) - 2.306499 * jax.random.uniform(key_of[2], (N_LOCAL, N_NODE * TOK_DEV, TOP), jnp.float32) ** shard_levels(key_of[2], (N_LOCAL, N_NODE * TOK_DEV, TOP), ((0, 32), (1, 32)), -0.2, 0.2)), 0.19921875, 2.0).astype(jnp.bfloat16)
    w_in = gaussian(key_of[3], (N_NODE * N_LOCAL, D // 2, 2 * FF_DEV), D ** -0.5, 0.0625, ((0, 1024),))
    w_out = gaussian(key_of[4], (N_NODE, FF, D), FF ** -0.5, 0.125, ((0, 32), (1, 32)))
    return dict(tokens=tokens, node_ids=node_ids, gates=gates, w_in=w_in, w_out=w_out)


def reference(tokens, node_ids, gates, w_in, w_out):
    count_all = N_LOCAL * N_NODE * TOK_DEV
    flat_tokens = tokens.reshape(count_all, D)
    flat_ids = node_ids.reshape(count_all, NODE_TOP)
    pair_gates = gates.reshape(count_all, NODE_TOP, 2).astype(jnp.float32)
    width = N_LOCAL * RECV
    half = D // 2
    split = N_LOCAL // 2
    ff_dev = FF // split
    block = FF // N_LOCAL
    positions = jnp.arange(count_all, dtype=jnp.int32)

    def one_expert(expert, total):
        expert = jnp.asarray(expert).astype(jnp.int32)
        group = expert // 2
        side = expert % 2
        hits = flat_ids == group
        visits = jnp.any(hits, axis=1)
        chosen = lax.dynamic_index_in_dim(pair_gates, side, 2, keepdims=False)
        weight = jnp.sum(jnp.where(hits, chosen, jnp.float32(0.0)), axis=1)
        order = jnp.cumsum(visits.astype(jnp.int32)) - 1
        target = jnp.where(visits, order, width).astype(jnp.int32)
        picked = jnp.zeros((width,), jnp.int32).at[target].set(positions, mode="drop")
        valid = jnp.arange(width, dtype=jnp.int32) < jnp.sum(visits.astype(jnp.int32))
        rows = flat_tokens[picked]
        row_gate = jnp.where(valid, weight[picked], jnp.float32(0.0))
        inner = lax.dynamic_slice_in_dim(w_in, (expert * N_LOCAL).astype(jnp.int32), N_LOCAL, 0)
        inner = inner.reshape(split, 2, half, 2, ff_dev).transpose(3, 1, 2, 0, 4).reshape(2, D, FF)
        gate_pre = jnp.dot(rows, inner[0], preferred_element_type=jnp.float32)
        up_pre = jnp.dot(rows, inner[1], preferred_element_type=jnp.float32)
        hidden = (row_gate[:, None] * jax.nn.silu(gate_pre) * up_pre).astype(jnp.bfloat16)
        outer = lax.dynamic_index_in_dim(w_out, expert, 0, keepdims=False).reshape(N_LOCAL, block, D)

        def add_block(index, acc):
            index = jnp.asarray(index).astype(jnp.int32)
            piece = lax.dynamic_slice_in_dim(hidden, (index * block).astype(jnp.int32), block, 1)
            weights = lax.dynamic_index_in_dim(outer, index, 0, keepdims=False)
            term = jnp.dot(piece, weights, preferred_element_type=jnp.float32).astype(jnp.bfloat16)
            term = lax.optimization_barrier(term)
            return acc + term.astype(jnp.float32)

        summed = lax.fori_loop(0, N_LOCAL, add_block, jnp.zeros((width, D), jnp.float32))
        node_out = lax.optimization_barrier(summed.astype(jnp.bfloat16)).astype(jnp.float32)
        node_out = jnp.where(valid[:, None], node_out, jnp.float32(0.0))
        return total.at[picked].add(node_out)

    total = lax.fori_loop(0, N_NODE, one_expert, jnp.zeros((count_all, D), jnp.float32))
    mixed = total.astype(jnp.bfloat16).reshape(N_LOCAL, N_NODE * TOK_DEV, D)
    member = flat_ids[:, :, None] == jnp.arange(N_NODE // 2, dtype=jnp.int32)
    group_count = jnp.sum(member.astype(jnp.float32), axis=(0, 1))
    counted = jnp.repeat(group_count, 2)
    gate_total = jnp.sum(jnp.where(member[:, :, :, None], pair_gates[:, :, None, :], jnp.float32(0.0)), axis=(0, 1)).reshape(N_NODE)
    scale = jnp.float32(N_NODE / (2 * NODE_TOP * count_all))
    balance = (counted * scale) * (gate_total * scale)
    return mixed, balance
```

```python
import functools

import jax
import jax.numpy as jnp
import numpy as np
from jax import lax
from jax.experimental import pallas as pl
from jax.experimental.pallas import tpu as pltpu
from jax.sharding import Mesh
from jax.sharding import PartitionSpec as P

F32 = jnp.float32
BF16 = jnp.bfloat16

NZ, NC, NY, NXH, NXL = 16, 2, 8, 2, 2
NX = NXH * NXL
AXES = ("z", "c", "y", "xh", "xl")
COLUMN = ("z", "c")
PLANE = ("y", "xh", "xl")
ROW = ("c", "xh", "xl")

LANES = 128
SLOTS = 9
EIGHTH = 7
HALF = NX * EIGHTH
TOK = 32
IN_ROWS = SLOTS * (EIGHTH + 1)
OUT_ROWS = 64
ROWS = NY * NX * SLOTS
PAIR = ROWS // 4
BLOCK = 64
WIDTH = EIGHTH * LANES


def swap_halves(v):
    return pltpu.roll(v, LANES // 2, 1)


def left_half(shape):
    return lax.broadcasted_iota(jnp.int32, shape, 1) < LANES // 2


def one_hot(row_key, col_key):
    return (row_key == col_key).astype(F32).astype(BF16)


def dot(a, b):
    return jnp.dot(a, b, preferred_element_type=F32)


def dot_t(a, b):
    return lax.dot_general(a, b, (((1,), (1,)), ((), ())), preferred_element_type=F32)


def call(body, outs, ins, scratch=(), smem=(), flops=10**8, limit=24 * 2**20):
    return pl.pallas_call(
        body,
        out_shape=outs,
        in_specs=[
            pl.BlockSpec(memory_space=pltpu.SMEM if i in smem else pltpu.VMEM)
            for i in range(len(ins))
        ],
        out_specs=jax.tree.map(lambda _: pl.BlockSpec(memory_space=pltpu.VMEM), outs),
        scratch_shapes=list(scratch),
        compiler_params=pltpu.CompilerParams(vmem_limit_bytes=limit),
        cost_estimate=pl.CostEstimate(flops=flops, bytes_accessed=10**6, transcendentals=0),
    )(*ins)


def spread_body(ids, gates, token, pick, out):
    base = dot(pick[...], token[...])
    row = lax.broadcasted_iota(jnp.int32, base.shape, 0)
    gate_row = lax.rem(row, TOK) == HALF
    left = left_half(base.shape)
    for z in range(NZ):
        live = jnp.float32(0.0)
        first = jnp.float32(0.0)
        second = jnp.float32(0.0)
        for m in range(4):
            hit = ids[m] == z
            live = jnp.where(hit, jnp.float32(1.0), live)
            first = jnp.where(hit, gates[2 * m], first)
            second = jnp.where(hit, gates[2 * m + 1], second)
        rows = jnp.where(live > 0, base, 0.0)
        rows = jnp.where(gate_row, jnp.where(left, first, second), rows)
        out[2 * TOK * z : 2 * TOK * (z + 1), :] = rows.astype(BF16)


def slot_of(gate_rows):
    live = (gate_rows > 0).astype(F32)
    a = lax.broadcasted_iota(jnp.int32, (TOK, TOK), 0)
    b = lax.broadcasted_iota(jnp.int32, (TOK, TOK), 1)
    order = dot((b <= a).astype(F32).astype(BF16), live.astype(BF16)) - 1.0
    return jnp.where(live > 0, order, 15.0)


def pack_body(arrived, row_key, out, gate_out):
    a = lax.broadcasted_iota(jnp.int32, (TOK, TOK * TOK), 0)
    b = lax.broadcasted_iota(jnp.int32, (TOK, TOK * TOK), 1)
    gate_rows = dot(one_hot(a * TOK + HALF, b), arrived[...])
    gate_out[...] = gate_rows
    slot = slot_of(gate_rows)
    lane = lax.broadcasted_iota(jnp.int32, (8, LANES), 1)
    by_token = dot_t(one_hot(lane, 0), slot.astype(BF16))
    token_of = lax.shift_right_logical(b, 5)
    spread = dot(by_token.astype(BF16), one_hot(a, token_of))
    chunk = lax.bitwise_and(b[0:1], TOK - 1).astype(F32)
    col_key = chunk * 16.0 + spread[0:1]
    packed = dot(one_hot(row_key[...], col_key), arrived[...]).astype(BF16)
    for y in range(NY):
        out[y * NX * IN_ROWS : (y + 1) * NX * IN_ROWS, :] = packed


def up_body(core, rows, place, w, out, gate_out, balance_out, x):
    n = 2 * NX * IN_ROWS
    a = lax.broadcasted_iota(jnp.int32, (n, n), 0)
    p = one_hot(a, place[...])
    for g in range(4):
        moved = dot(p, rows[n * g : n * (g + 1), :])
        for k in range(EIGHTH + 1):
            x[k, PAIR * g : PAIR * (g + 1), :] = moved[PAIR * k : PAIR * (k + 1), :]
    gate = x[EIGHTH]
    gate = jnp.where(core[0] == 0, gate, swap_halves(gate))
    gate_out[...] = gate
    count = jnp.sum((gate > 0).astype(F32), axis=0, keepdims=True)
    total = jnp.sum(gate, axis=0, keepdims=True)
    scale = jnp.float32(1.0 / 256.0)
    balance_out[...] = jnp.broadcast_to((count * scale) * (total * scale), (8, LANES))
    features = jnp.concatenate([x[k].astype(BF16) for k in range(EIGHTH)], axis=1)
    left = left_half((ROWS, LANES))
    for j in range(4):
        both = dot(features, w[WIDTH * j : WIDTH * (j + 1), :])
        g, u = both[:, :LANES], both[:, LANES:]
        out[ROWS * 2 * j : ROWS * (2 * j + 1), :] = jnp.where(left, g, swap_halves(u)).astype(BF16)
        out[ROWS * (2 * j + 1) : ROWS * (2 * j + 2), :] = jnp.where(left, swap_halves(g), u).astype(BF16)


def hidden_body(parts, gate, out):
    total = parts[0:ROWS, :].astype(F32)
    for j in range(1, 8):
        total = total + parts[ROWS * j : ROWS * (j + 1), :].astype(F32)
    up = swap_halves(total)
    h = gate[...] * (total / (1.0 + jnp.exp(-total))) * up
    half = ROWS // 2
    h = jnp.where(left_half((half, LANES)), h[:half], swap_halves(h[half:])).astype(BF16)
    for j in range(8):
        out[half * j : half * (j + 1), :] = h


def down_body(hidden, w, place, out, acc):
    half = ROWS // 2
    left = left_half((half, LANES))
    top, bottom = [], []
    for j in range(0, 8, 2):
        a = hidden[half * j : half * (j + 1), :].astype(F32)
        b = hidden[half * (j + 1) : half * (j + 2), :].astype(F32)
        top.append(jnp.where(left, a, swap_halves(b)).astype(BF16))
        bottom.append(jnp.where(left, swap_halves(a), b).astype(BF16))
    acc[0:half, :] = dot(jnp.concatenate(top, axis=1), w[...])
    acc[half:ROWS, :] = dot(jnp.concatenate(bottom, axis=1), w[...])
    n = 2 * NX * OUT_ROWS
    a = lax.broadcasted_iota(jnp.int32, (n, EIGHTH * PAIR), 0)
    q = one_hot(a, place[...])
    for g in range(4):
        stacked = jnp.concatenate(
            [acc[PAIR * g : PAIR * (g + 1), LANES * k : LANES * (k + 1)] for k in range(EIGHTH)],
            axis=0,
        ).astype(BF16)
        out[n * g : n * (g + 1), :] = dot(q, stacked).astype(BF16)


def unpack_body(parts, gate_rows, col_key, out):
    n = NX * OUT_ROWS
    total = parts[0:n, :].astype(F32)
    for y in range(1, NY):
        total = total + parts[n * y : n * (y + 1), :].astype(F32)
    slot = slot_of(gate_rows[...])
    a = lax.broadcasted_iota(jnp.int32, (TOK * TOK, TOK), 0)
    b = lax.broadcasted_iota(jnp.int32, (TOK * TOK, TOK), 1)
    spread = dot(one_hot(lax.shift_right_logical(a, 5), b), slot.astype(BF16))
    chunk = lax.bitwise_and(lax.broadcasted_iota(jnp.int32, (TOK * TOK, LANES), 0), TOK - 1)
    key = (chunk.astype(F32) * 16.0 + spread)[:, 0:1]
    out[...] = dot(one_hot(key, col_key[...]), total.astype(BF16)).astype(BF16)


def finish_body(parts, pick, out):
    n = 2 * TOK
    total = parts[0:n, :].astype(F32)
    for z in range(1, NZ):
        total = total + parts[n * z : n * (z + 1), :].astype(F32)
    out[...] = dot(pick[...], total.astype(BF16)).astype(BF16)


@functools.cache
def tables():
    spread_pick = np.zeros((2 * TOK, 2 * HALF), np.float32)
    for c in range(NC):
        for xh in range(NXH):
            for xl in range(NXL):
                for k in range(EIGHTH):
                    j = (xh * NXL + xl) * EIGHTH + k
                    spread_pick[c * TOK + j, xl * HALF + (c * NXH + xh) * EIGHTH + k] = 1
    pack_key = np.zeros((NX * IN_ROWS, 1), np.float32)
    for x in range(NX):
        for k in range(EIGHTH + 1):
            for r in range(SLOTS):
                chunk = x * EIGHTH + k if k < EIGHTH else HALF
                pack_key[x * IN_ROWS + k * SLOTS + r, 0] = chunk * 16 + r
    cols = 2 * NX
    up_place = np.zeros((1, cols * IN_ROWS), np.int32)
    down_place = np.zeros((1, EIGHTH * PAIR), np.int32)
    for col in range(cols):
        for k in range(EIGHTH + 1):
            for r in range(SLOTS):
                up_place[0, col * IN_ROWS + k * SLOTS + r] = k * PAIR + col * SLOTS + r
                if k < EIGHTH:
                    down_place[0, k * PAIR + col * SLOTS + r] = col * OUT_ROWS + k * SLOTS + r
    unpack_key = np.full((1, NX * OUT_ROWS), -1, np.float32)
    for x in range(NX):
        for k in range(EIGHTH):
            for r in range(SLOTS):
                unpack_key[0, x * OUT_ROWS + k * SLOTS + r] = (x * EIGHTH + k) * 16 + r
    finish_pick = np.zeros((2 * HALF, 2 * TOK), np.float32)
    for c in range(NC):
        for j in range(HALF):
            finish_pick[c * HALF + j, c * TOK + j] = 1
    return spread_pick, pack_key, up_place, down_place, unpack_key, finish_pick


def exchange(x, axes, members):
    rows = x.shape[0] // members
    y = lax.all_to_all(
        x.reshape(members, rows, x.shape[1]), axes, split_axis=0, concat_axis=0, tiled=True
    )
    return y.reshape(x.shape)


def shards(tokens, node_ids, gates, w_in, w_out):
    spread_pick, pack_key, up_place, down_place, unpack_key, finish_pick = tables()
    shape = jax.ShapeDtypeStruct
    core = lax.axis_index("c").astype(jnp.int32).reshape(1)

    sent = call(
        spread_body,
        shape((TOK * TOK, LANES), BF16),
        (
            node_ids.reshape(4),
            gates.reshape(8).astype(F32),
            tokens.reshape(2 * HALF, LANES),
            jnp.asarray(spread_pick, BF16),
        ),
        smem=(0, 1),
    )
    arrived = exchange(sent, COLUMN, NZ * NC)
    w_up = exchange(w_in.reshape(4 * WIDTH, 2 * LANES), ("c", "xh"), NC * NXH)
    w_down = w_out.reshape(BLOCK, 8, WIDTH).transpose(1, 0, 2).reshape(8 * BLOCK, WIDTH)
    w_down = exchange(w_down, ROW, 8)

    packed, gate_rows = call(
        pack_body,
        (shape((NY * NX * IN_ROWS, LANES), BF16), shape((TOK, LANES), F32)),
        (arrived, jnp.asarray(pack_key)),
    )
    rows = exchange(packed, PLANE, NY * NX)

    partial_sums, gate, balance = call(
        up_body,
        (shape((8 * ROWS, LANES), BF16), shape((ROWS, LANES), F32), shape((8, LANES), F32)),
        (core, rows, jnp.asarray(up_place), w_up),
        scratch=(pltpu.VMEM((EIGHTH + 1, ROWS, LANES), F32),),
        smem=(0,),
        flops=10**9,
    )
    summands = exchange(partial_sums, ROW, 8)

    hidden = call(hidden_body, shape((4 * ROWS, LANES), BF16), (summands, gate))
    every_hidden = exchange(hidden, ROW, 8)

    down = call(
        down_body,
        shape((NY * NX * OUT_ROWS, LANES), BF16),
        (every_hidden, w_down, jnp.asarray(down_place)),
        scratch=(pltpu.VMEM((ROWS, WIDTH), F32),),
        flops=10**9,
    )
    returned = exchange(down, PLANE, NY * NX)

    unpacked = call(
        unpack_body,
        shape((TOK * TOK, LANES), BF16),
        (returned, gate_rows, jnp.asarray(unpack_key)),
    )
    back = exchange(unpacked, COLUMN, NZ * NC)

    mixed = call(
        finish_body,
        shape((2 * HALF, LANES), BF16),
        (back, jnp.asarray(finish_pick, BF16)),
    )
    return mixed.reshape(1, 1, 2 * HALF * LANES), balance[0, 0:1]


def solution(mesh):
    fine = Mesh(mesh.devices.reshape(NZ, NC, NY, NXH, NXL), AXES)
    token_spec = P(PLANE, COLUMN, None)
    return jax.shard_map(
        shards,
        mesh=fine,
        in_specs=(
            token_spec,
            token_spec,
            token_spec,
            P(AXES, None, None),
            P(COLUMN, PLANE, None),
        ),
        out_specs=(token_spec, P(COLUMN)),
        check_vma=False,
    )
```

```python
import functools

import jax
import jax.numpy as jnp
import numpy as np
from jax import lax
from jax.experimental import pallas as pl
from jax.experimental.pallas import tpu as pltpu
from jax.sharding import Mesh
from jax.sharding import PartitionSpec as P


F32 = jnp.float32
BF16 = jnp.bfloat16

NZ, NC, NY, NXH, NXL = 16, 2, 8, 2, 2
NX = NXH * NXL
AXES = ("z", "c", "y", "xh", "xl")
COLUMN = ("z", "c")
PLANE = ("y", "xh", "xl")
ROW = ("c", "xh", "xl")

LANES = 128
SLOTS = 9
EIGHTH = 7
HALF = NX * EIGHTH
TOK = 32
IN_ROWS = SLOTS * (EIGHTH + 1)
OUT_ROWS = 64
ROWS = NY * NX * SLOTS
PAIR = ROWS // 4
BLOCK = 64
WIDTH = EIGHTH * LANES


def swap_halves(v):
    return pltpu.roll(v, LANES // 2, 1)


def left_half(shape):
    return lax.broadcasted_iota(jnp.int32, shape, 1) < LANES // 2


def one_hot(row_key, col_key):
    return (row_key == col_key).astype(F32).astype(BF16)


def dot(a, b):
    return jnp.dot(a, b, preferred_element_type=F32)


def dot_t(a, b):
    return lax.dot_general(a, b, (((1,), (1,)), ((), ())), preferred_element_type=F32)


def call(body, outs, ins, scratch=(), smem=(), flops=10**8, limit=24 * 2**20):
    return pl.pallas_call(
        body,
        out_shape=outs,
        in_specs=[
            pl.BlockSpec(memory_space=pltpu.SMEM if i in smem else pltpu.VMEM)
            for i in range(len(ins))
        ],
        out_specs=jax.tree.map(lambda _: pl.BlockSpec(memory_space=pltpu.VMEM), outs),
        scratch_shapes=list(scratch),
        compiler_params=pltpu.CompilerParams(vmem_limit_bytes=limit),
        cost_estimate=pl.CostEstimate(flops=flops, bytes_accessed=10**6, transcendentals=0),
    )(*ins)


def spread_body(ids, gates, token, pick, out):
    base = dot(pick[...], token[...])
    row = lax.broadcasted_iota(jnp.int32, base.shape, 0)
    gate_row = lax.rem(row, TOK) == HALF
    left = left_half(base.shape)
    for z in range(NZ):
        live = jnp.float32(0.0)
        first = jnp.float32(0.0)
        second = jnp.float32(0.0)
        for m in range(4):
            hit = ids[m] == z
            live = jnp.where(hit, jnp.float32(1.0), live)
            first = jnp.where(hit, gates[2 * m], first)
            second = jnp.where(hit, gates[2 * m + 1], second)
        rows = jnp.where(live > 0, base, 0.0)
        rows = jnp.where(gate_row, jnp.where(left, first, second), rows)
        out[2 * TOK * z : 2 * TOK * (z + 1), :] = rows.astype(BF16)


def slot_of(gate_rows):
    live = (gate_rows > 0).astype(F32)
    a = lax.broadcasted_iota(jnp.int32, (TOK, TOK), 0)
    b = lax.broadcasted_iota(jnp.int32, (TOK, TOK), 1)
    order = dot((b <= a).astype(F32).astype(BF16), live.astype(BF16)) - 1.0
    return jnp.where(live > 0, order, 15.0)


def pack_body(arrived, row_key, out, gate_out):
    a = lax.broadcasted_iota(jnp.int32, (TOK, TOK * TOK), 0)
    b = lax.broadcasted_iota(jnp.int32, (TOK, TOK * TOK), 1)
    gate_rows = dot(one_hot(a * TOK + HALF, b), arrived[...])
    gate_out[...] = gate_rows
    slot = slot_of(gate_rows)
    lane = lax.broadcasted_iota(jnp.int32, (8, LANES), 1)
    by_token = dot_t(one_hot(lane, 0), slot.astype(BF16))
    token_of = lax.shift_right_logical(b, 5)
    spread = dot(by_token.astype(BF16), one_hot(a, token_of))
    chunk = lax.bitwise_and(b[0:1], TOK - 1).astype(F32)
    col_key = chunk * 16.0 + spread[0:1]
    packed = dot(one_hot(row_key[...], col_key), arrived[...]).astype(BF16)
    for y in range(NY):
        out[y * NX * IN_ROWS : (y + 1) * NX * IN_ROWS, :] = packed


def up_body(place_ids, rows, place, w_here, w_there, out, gate_out, balance_out, x):
    core, xh = place_ids[0], place_ids[1]
    n = 2 * NX * IN_ROWS
    a = lax.broadcasted_iota(jnp.int32, (n, n), 0)
    p = one_hot(a, place[...])
    for g in range(4):
        moved = dot(p, rows[n * g : n * (g + 1), :])
        for k in range(EIGHTH + 1):
            x[k, PAIR * g : PAIR * (g + 1), :] = moved[PAIR * k : PAIR * (k + 1), :]
    gate = x[EIGHTH]
    gate = jnp.where(core == 0, gate, swap_halves(gate))
    gate_out[...] = gate
    count = jnp.sum((gate > 0).astype(F32), axis=0, keepdims=True)
    total = jnp.sum(gate, axis=0, keepdims=True)
    scale = jnp.float32(1.0 / 256.0)
    balance_out[...] = jnp.broadcast_to((count * scale) * (total * scale), (8, LANES))
    features = jnp.concatenate([x[k].astype(BF16) for k in range(EIGHTH)], axis=1)
    left = left_half((ROWS, LANES))
    for j in range(4):
        w = (w_here, w_there)[j // 2]
        both = dot(features, w[WIDTH * (j % 2) : WIDTH * (j % 2 + 1), :])
        g, u = both[:, :LANES], both[:, LANES:]
        expert = core if j % 2 == 0 else 1 - core
        part = xh if j < 2 else 1 - xh
        at = ROWS * 2 * (expert * NXH + part)
        out[pl.ds(pl.multiple_of(at, ROWS), ROWS), :] = jnp.where(left, g, swap_halves(u)).astype(BF16)
        at = at + ROWS
        out[pl.ds(pl.multiple_of(at, ROWS), ROWS), :] = jnp.where(left, swap_halves(g), u).astype(BF16)


def hidden_body(parts, gate, out):
    total = parts[0:ROWS, :].astype(F32)
    for j in range(1, 8):
        total = total + parts[ROWS * j : ROWS * (j + 1), :].astype(F32)
    up = swap_halves(total)
    h = gate[...] * (total / (1.0 + jnp.exp(-total))) * up
    half = ROWS // 2
    h = jnp.where(left_half((half, LANES)), h[:half], swap_halves(h[half:])).astype(BF16)
    for j in range(8):
        out[half * j : half * (j + 1), :] = h


def down_body(place_ids, hidden, w0, w1, w2, w3, place, out, acc):
    core, x = place_ids[0], place_ids[2]
    half = ROWS // 2
    left = left_half((half, LANES))

    def block(expert, source):
        at = pl.multiple_of((expert * NX + source) * half, half)
        return hidden[pl.ds(at, half), :].astype(F32)

    for d, w in enumerate((w0, w1, w2, w3)):
        source = lax.bitwise_xor(x, jnp.int32(d))
        a, b = block(core, source), block(1 - core, source)
        top = dot(jnp.where(left, a, swap_halves(b)).astype(BF16), w[...])
        bottom = dot(jnp.where(left, swap_halves(a), b).astype(BF16), w[...])
        if d == 0:
            acc[0:half, :] = top
            acc[half:ROWS, :] = bottom
        else:
            acc[0:half, :] += top
            acc[half:ROWS, :] += bottom
    n = 2 * NX * OUT_ROWS
    a = lax.broadcasted_iota(jnp.int32, (n, EIGHTH * PAIR), 0)
    q = one_hot(a, place[...])
    for g in range(4):
        stacked = jnp.concatenate(
            [acc[PAIR * g : PAIR * (g + 1), LANES * k : LANES * (k + 1)] for k in range(EIGHTH)],
            axis=0,
        ).astype(BF16)
        out[n * g : n * (g + 1), :] = dot(q, stacked).astype(BF16)


def unpack_body(parts, gate_rows, col_key, out):
    n = NX * OUT_ROWS
    total = parts[0:n, :].astype(F32)
    for y in range(1, NY):
        total = total + parts[n * y : n * (y + 1), :].astype(F32)
    slot = slot_of(gate_rows[...])
    a = lax.broadcasted_iota(jnp.int32, (TOK * TOK, TOK), 0)
    b = lax.broadcasted_iota(jnp.int32, (TOK * TOK, TOK), 1)
    spread = dot(one_hot(lax.shift_right_logical(a, 5), b), slot.astype(BF16))
    chunk = lax.bitwise_and(lax.broadcasted_iota(jnp.int32, (TOK * TOK, LANES), 0), TOK - 1)
    key = (chunk.astype(F32) * 16.0 + spread)[:, 0:1]
    out[...] = dot(one_hot(key, col_key[...]), total.astype(BF16)).astype(BF16)


def finish_body(parts, pick, out):
    n = 2 * TOK
    total = parts[0:n, :].astype(F32)
    for z in range(1, NZ):
        total = total + parts[n * z : n * (z + 1), :].astype(F32)
    out[...] = dot(pick[...], total.astype(BF16)).astype(BF16)


@functools.cache
def tables():
    spread_pick = np.zeros((2 * TOK, 2 * HALF), np.float32)
    for c in range(NC):
        for xh in range(NXH):
            for xl in range(NXL):
                for k in range(EIGHTH):
                    j = (xh * NXL + xl) * EIGHTH + k
                    spread_pick[c * TOK + j, xl * HALF + (c * NXH + xh) * EIGHTH + k] = 1
    pack_key = np.zeros((NX * IN_ROWS, 1), np.float32)
    for x in range(NX):
        for k in range(EIGHTH + 1):
            for r in range(SLOTS):
                chunk = x * EIGHTH + k if k < EIGHTH else HALF
                pack_key[x * IN_ROWS + k * SLOTS + r, 0] = chunk * 16 + r
    cols = 2 * NX
    up_place = np.zeros((1, cols * IN_ROWS), np.int32)
    down_place = np.zeros((1, EIGHTH * PAIR), np.int32)
    for col in range(cols):
        for k in range(EIGHTH + 1):
            for r in range(SLOTS):
                up_place[0, col * IN_ROWS + k * SLOTS + r] = k * PAIR + col * SLOTS + r
                if k < EIGHTH:
                    down_place[0, k * PAIR + col * SLOTS + r] = col * OUT_ROWS + k * SLOTS + r
    unpack_key = np.full((1, NX * OUT_ROWS), -1, np.float32)
    for x in range(NX):
        for k in range(EIGHTH):
            for r in range(SLOTS):
                unpack_key[0, x * OUT_ROWS + k * SLOTS + r] = (x * EIGHTH + k) * 16 + r
    finish_pick = np.zeros((2 * HALF, 2 * TOK), np.float32)
    for c in range(NC):
        for j in range(HALF):
            finish_pick[c * HALF + j, c * TOK + j] = 1
    return spread_pick, pack_key, up_place, down_place, unpack_key, finish_pick


def exchange(x, axes, members):
    rows = x.shape[0] // members
    y = lax.all_to_all(
        x.reshape(members, rows, x.shape[1]), axes, split_axis=0, concat_axis=0, tiled=True
    )
    return y.reshape(x.shape)


def swapped(x, axis):
    return lax.ppermute(x, axis, [(0, 1), (1, 0)])


def x_swapped(x, mask):
    return lax.ppermute(x, ("xh", "xl"), [(i, i ^ mask) for i in range(NX)])


def rows_at(start, size):
    return pl.ds(pl.multiple_of(start, size), size)


def for_core_body(place_ids, w_in, w_out, up, down):
    other = 1 - place_ids[0]
    up[...] = w_in[rows_at(other * 2 * WIDTH, 2 * WIDTH), :]
    down[...] = w_out[:, rows_at(other * NX * WIDTH, NX * WIDTH)]


def for_row_body(place_ids, w_in, w_out, up, down, up_here, up_there, d0, d1, d2, d3):
    core, xh, x = place_ids[0], place_ids[1], place_ids[2]
    for out, side in ((up_here, xh), (up_there, 1 - xh)):
        out[0:WIDTH, :] = w_in[rows_at((2 * core + side) * WIDTH, WIDTH), :]
        out[WIDTH : 2 * WIDTH, :] = up[rows_at(side * WIDTH, WIDTH), :]
    for d, out in enumerate((d0, d1, d2, d3)):
        to = lax.bitwise_xor(x, jnp.int32(d))
        out[0:BLOCK, :] = w_out[:, rows_at((core * NX + to) * WIDTH, WIDTH)]
        out[BLOCK : 2 * BLOCK, :] = down[:, rows_at(to * WIDTH, WIDTH)]


def spread_weights(place_ids, w_in, w_out):
    shape = jax.ShapeDtypeStruct
    up_shape, down_shape = shape((2 * WIDTH, 2 * LANES), BF16), shape((2 * BLOCK, WIDTH), BF16)
    up, down = call(
        for_core_body,
        (up_shape, shape((BLOCK, NX * WIDTH), BF16)),
        (place_ids, w_in, w_out),
        smem=(0,),
    )
    up = swapped(up, "c")
    down = swapped(down, "c")
    up_here, up_there, *parts = call(
        for_row_body,
        (up_shape,) * 2 + (down_shape,) * NX,
        (place_ids, w_in, w_out, up, down),
        smem=(0,),
    )
    up_there = swapped(up_there, "xh")
    for d in range(1, NX):
        parts[d] = x_swapped(parts[d], d)
    return (up_here, up_there), parts


def layer(tokens, node_ids, gates, w_in, w_out):
    spread_pick, pack_key, up_place, down_place, unpack_key, finish_pick = tables()
    shape = jax.ShapeDtypeStruct
    core, xh, xl = (lax.axis_index(a).astype(jnp.int32) for a in ROW)
    place_ids = jnp.stack([core, xh, xh * NXL + xl])

    sent = call(
        spread_body,
        shape((TOK * TOK, LANES), BF16),
        (
            node_ids.reshape(4),
            gates.reshape(8).astype(F32),
            tokens.reshape(2 * HALF, LANES),
            jnp.asarray(spread_pick, BF16),
        ),
        smem=(0, 1),
    )
    sent, w_in, w_out = lax.optimization_barrier((sent, w_in, w_out))
    arrived = exchange(sent, COLUMN, NZ * NC)
    w_up, w_down = spread_weights(place_ids, w_in.reshape(4 * WIDTH, 2 * LANES), w_out[0])

    packed, gate_rows = call(
        pack_body,
        (shape((NY * NX * IN_ROWS, LANES), BF16), shape((TOK, LANES), F32)),
        (arrived, jnp.asarray(pack_key)),
    )
    rows = exchange(packed, PLANE, NY * NX)

    partial_sums, gate, balance = call(
        up_body,
        (shape((8 * ROWS, LANES), BF16), shape((ROWS, LANES), F32), shape((8, LANES), F32)),
        (place_ids, rows, jnp.asarray(up_place), *w_up),
        scratch=(pltpu.VMEM((EIGHTH + 1, ROWS, LANES), F32),),
        smem=(0,),
        flops=10**9,
    )
    summands = exchange(partial_sums, ROW, 8)

    hidden = call(hidden_body, shape((4 * ROWS, LANES), BF16), (summands, gate))
    every_hidden = exchange(hidden, ROW, 8)

    down = call(
        down_body,
        shape((NY * NX * OUT_ROWS, LANES), BF16),
        (place_ids, every_hidden, *w_down, jnp.asarray(down_place)),
        scratch=(pltpu.VMEM((ROWS, WIDTH), F32),),
        smem=(0,),
        flops=10**9,
    )
    returned = exchange(down, PLANE, NY * NX)

    unpacked = call(
        unpack_body,
        shape((TOK * TOK, LANES), BF16),
        (returned, gate_rows, jnp.asarray(unpack_key)),
    )
    back = exchange(unpacked, COLUMN, NZ * NC)

    mixed = call(
        finish_body,
        shape((2 * HALF, LANES), BF16),
        (back, jnp.asarray(finish_pick, BF16)),
    )
    return mixed.reshape(1, 1, 2 * HALF * LANES), balance[0, 0:1]


def solution(mesh):
    fine = Mesh(mesh.devices.reshape(NZ, NC, NY, NXH, NXL), AXES)
    token_spec = P(PLANE, COLUMN, None)
    return jax.shard_map(
        layer,
        mesh=fine,
        in_specs=(
            token_spec,
            token_spec,
            token_spec,
            P(AXES, None, None),
            P(COLUMN, PLANE, None),
        ),
        out_specs=(token_spec, P(COLUMN)),
        check_vma=False,
    )
```

```python
import jax
import jax.numpy as jnp
from jax import lax
from jax.experimental import pallas as pl
from jax.experimental.pallas import tpu as pltpu
from jax.sharding import Mesh
from jax.sharding import PartitionSpec as P


F32 = jnp.float32
BF16 = jnp.bfloat16

NZ, NC, NY, NXH, NXL = 16, 2, 8, 2, 2
NX = NXH * NXL
AXES = ("z", "c", "y", "xh", "xl")
COLUMN = ("z", "c")
PLANE = ("y", "xh", "xl")
ROW = ("c", "xh", "xl")

LANES = 128
SLOTS = 9
EIGHTH = 7
HALF = NX * EIGHTH
TOK = 32
BLOCK_ROWS = 64
ROWS = NY * NX * SLOTS
PAIR = ROWS // 4
BLOCK = 64
WIDTH = EIGHTH * LANES


def swap_halves(v):
    return pltpu.roll(v, LANES // 2, 1)


def left_half(shape):
    return lax.broadcasted_iota(jnp.int32, shape, 1) < LANES // 2


def one_hot(row_key, col_key):
    return (row_key == col_key).astype(F32).astype(BF16)


def iota(shape, axis):
    return lax.broadcasted_iota(jnp.int32, shape, axis).astype(F32)


def divided(value, by):
    quotient = jnp.floor((value + 0.5) * (1.0 / by))
    return quotient, value - by * quotient


def dot(a, b):
    return jnp.dot(a, b, preferred_element_type=F32)


def dot_t(a, b):
    return lax.dot_general(a, b, (((1,), (1,)), ((), ())), preferred_element_type=F32)


def call(body, outs, ins, scratch=(), smem=(), smem_out=(), far=False, flops=10**8, limit=24 * 2**20):
    def spec(in_smem):
        return pl.BlockSpec(memory_space=pltpu.SMEM if in_smem else pltpu.VMEM)

    far_spec = pl.BlockSpec(memory_space=pltpu.HBM)

    if far:
        ins = [pltpu.with_memory_space_constraint(x, pltpu.HBM) for x in ins]
    several = isinstance(outs, tuple)
    return pl.pallas_call(
        body,
        out_shape=outs,
        in_specs=[far_spec if far else spec(i in smem) for i in range(len(ins))],
        out_specs=tuple(spec(i in smem_out) for i in range(len(outs))) if several else spec(False),
        scratch_shapes=list(scratch),
        compiler_params=pltpu.CompilerParams(vmem_limit_bytes=limit),
        cost_estimate=pl.CostEstimate(flops=flops, bytes_accessed=10**6, transcendentals=0),
    )(*ins)


def spread_body(far_ids, far_gates, far_token, out, ids, gates, token, base, arrived):
    copies = [
        pltpu.make_async_copy(far, near, arrived.at[i])
        for i, (far, near) in enumerate(((far_token, token), (far_ids, ids), (far_gates, gates)))
    ]
    for copy in copies:
        copy.start()
    for copy in copies:
        copy.wait()
    for c in range(NC):
        for xh in range(NXH):
            for xl in range(NXL):
                for k in range(EIGHTH):
                    row = c * TOK + (xh * NXL + xl) * EIGHTH + k
                    i = xl * HALF + (c * NXH + xh) * EIGHTH + k
                    base[row : row + 1, :] = token[:, i * LANES : (i + 1) * LANES].astype(F32)
        base[c * TOK + HALF : (c + 1) * TOK, :] = jnp.zeros((TOK - HALF, LANES), F32)
    tile = (8, LANES)
    left = left_half(tile)
    gate_row = lax.broadcasted_iota(jnp.int32, tile, 0) == HALF % 8
    every_gate = gates[...].astype(F32)
    nodes, pairs = [], []
    for m in range(4):
        nodes.append(jnp.broadcast_to(ids[:, m : m + 1], tile))
        first = jnp.broadcast_to(every_gate[:, 2 * m : 2 * m + 1], tile)
        second = jnp.broadcast_to(every_gate[:, 2 * m + 1 : 2 * m + 2], tile)
        pairs.append(jnp.where(left, first, second))
    blocks = [base[8 * b : 8 * (b + 1), :] for b in range(2 * TOK // 8)]
    for z in range(NZ):
        gate = jnp.zeros(tile, F32)
        for node, pair in zip(nodes, pairs):
            gate = jnp.where(node == z, pair, gate)
        live = gate > 0
        rows = [jnp.where(live, block, 0.0) for block in blocks]
        for b in (HALF // 8, (TOK + HALF) // 8):
            rows[b] = jnp.where(gate_row, gate, rows[b])
        out[2 * TOK * z : 2 * TOK * (z + 1), :] = jnp.concatenate(rows, axis=0).astype(BF16)


def slot_of(gate_rows):
    live = (gate_rows > 0).astype(F32)
    a = lax.broadcasted_iota(jnp.int32, (TOK, TOK), 0)
    b = lax.broadcasted_iota(jnp.int32, (TOK, TOK), 1)
    order = dot((b <= a).astype(F32).astype(BF16), live.astype(BF16)) - 1.0
    return jnp.where(live > 0, order, 15.0)


def chunk_and_slot(at):
    x, row = divided(at, BLOCK_ROWS)
    k, r = divided(row, SLOTS)
    return jnp.where(k < EIGHTH, (x * EIGHTH + k) * 16.0 + r, -1.0)


def pack_body(arrived, out, gate_out):
    a = lax.broadcasted_iota(jnp.int32, (TOK, TOK * TOK), 0)
    b = lax.broadcasted_iota(jnp.int32, (TOK, TOK * TOK), 1)
    gate_rows = dot(one_hot(a * TOK + HALF, b), arrived[...])
    gate_out[...] = gate_rows
    slot = slot_of(gate_rows)
    lane = lax.broadcasted_iota(jnp.int32, (8, LANES), 1)
    by_token = dot_t(one_hot(lane, 0), slot.astype(BF16))
    token_of = lax.shift_right_logical(b, 5)
    spread = dot(by_token.astype(BF16), one_hot(a, token_of))
    chunk = lax.bitwise_and(b[0:1], TOK - 1).astype(F32)
    col_key = chunk * 16.0 + spread[0:1]
    row_key = chunk_and_slot(iota((NX * BLOCK_ROWS, 1), 0))
    packed = dot(one_hot(row_key, col_key), arrived[...])
    lane = lax.broadcasted_iota(jnp.int32, (TOK, LANES), 1)
    wanted = lax.bitwise_and(lane, 15).astype(F32) == slot
    value = jnp.where(lane < 16, gate_rows, jnp.where(lane < 32, swap_halves(gate_rows), 0.0))
    gate_line = jnp.sum(jnp.where(wanted, value, 0.0), axis=0, keepdims=True)
    row = lax.broadcasted_iota(jnp.int32, packed.shape, 0)
    last = lax.bitwise_and(row, BLOCK_ROWS - 1) == BLOCK_ROWS - 1
    packed = jnp.where(last, gate_line, packed).astype(BF16)
    for y in range(NY):
        out[y * NX * BLOCK_ROWS : (y + 1) * NX * BLOCK_ROWS, :] = packed


def up_body(place_ids, rows, w_here, w_there, out, gate_out, balance_out, x):
    core, xh = place_ids[0], place_ids[1]
    n = 2 * NX * BLOCK_ROWS
    column, row = divided(iota((1, n), 1), BLOCK_ROWS)
    k, r = divided(row, SLOTS)
    of_pair, _ = divided(iota((PAIR, 1), 0), SLOTS)
    p = jnp.concatenate(
        [
            one_hot(iota((EIGHTH * PAIR, n), 0), k * PAIR + column * SLOTS + r),
            one_hot((of_pair + 1.0) * BLOCK_ROWS - 1.0, iota((PAIR, n), 1)),
        ],
        axis=0,
    )
    for g in range(4):
        moved = dot(p, rows[n * g : n * (g + 1), :])
        for k in range(EIGHTH + 1):
            x[k, PAIR * g : PAIR * (g + 1), :] = moved[PAIR * k : PAIR * (k + 1), :]
    _, slot = divided(iota((ROWS, 1), 0), SLOTS)
    wanted = iota((ROWS, LANES), 1) == slot + 16.0 * core.astype(F32)
    gate = jnp.sum(jnp.where(wanted, x[EIGHTH], 0.0), axis=1, keepdims=True)
    gate_out[...] = jnp.broadcast_to(gate, (ROWS, LANES))
    scale = jnp.float32(1.0 / 256.0)
    count, total = jnp.sum((gate > 0).astype(F32)), jnp.sum(gate)
    balance_out[0] = (count * scale) * (total * scale)
    features = jnp.concatenate([x[k].astype(BF16) for k in range(EIGHTH)], axis=1)
    left = left_half((ROWS, LANES))
    for j in range(4):
        w = (w_here, w_there)[j // 2]
        both = dot(features, w[WIDTH * (j % 2) : WIDTH * (j % 2 + 1), :])
        g, u = both[:, :LANES], both[:, LANES:]
        expert = core if j % 2 == 0 else 1 - core
        part = xh if j < 2 else 1 - xh
        at = ROWS * 2 * (expert * NXH + part)
        out[pl.ds(pl.multiple_of(at, ROWS), ROWS), :] = jnp.where(left, g, swap_halves(u)).astype(BF16)
        at = at + ROWS
        out[pl.ds(pl.multiple_of(at, ROWS), ROWS), :] = jnp.where(left, swap_halves(g), u).astype(BF16)


def hidden_body(parts, gate, out):
    total = parts[0:ROWS, :].astype(F32)
    for j in range(1, 8):
        total = total + parts[ROWS * j : ROWS * (j + 1), :].astype(F32)
    up = swap_halves(total)
    h = gate[...] * (total / (1.0 + jnp.exp(-total))) * up
    half = ROWS // 2
    h = jnp.where(left_half((half, LANES)), h[:half], swap_halves(h[half:])).astype(BF16)
    for j in range(8):
        out[half * j : half * (j + 1), :] = h


def down_body(place_ids, hidden, w0, w1, w2, w3, out, acc):
    core, x = place_ids[0], place_ids[2]
    half = ROWS // 2
    left = left_half((half, LANES))

    def block(expert, source):
        at = pl.multiple_of((expert * NX + source) * half, half)
        return hidden[pl.ds(at, half), :].astype(F32)

    for d, w in enumerate((w0, w1, w2, w3)):
        source = lax.bitwise_xor(x, jnp.int32(d))
        a, b = block(core, source), block(1 - core, source)
        top = dot(jnp.where(left, a, swap_halves(b)).astype(BF16), w[...])
        bottom = dot(jnp.where(left, swap_halves(a), b).astype(BF16), w[...])
        if d == 0:
            acc[0:half, :] = top
            acc[half:ROWS, :] = bottom
        else:
            acc[0:half, :] += top
            acc[half:ROWS, :] += bottom
    n = 2 * NX * BLOCK_ROWS
    k, row = divided(iota((1, EIGHTH * PAIR), 1), PAIR)
    column, r = divided(row, SLOTS)
    q = one_hot(iota((n, EIGHTH * PAIR), 0), column * BLOCK_ROWS + k * SLOTS + r)
    for g in range(4):
        stacked = jnp.concatenate(
            [acc[PAIR * g : PAIR * (g + 1), LANES * k : LANES * (k + 1)] for k in range(EIGHTH)],
            axis=0,
        ).astype(BF16)
        out[n * g : n * (g + 1), :] = dot(q, stacked).astype(BF16)


def unpack_body(parts, gate_rows, out):
    n = NX * BLOCK_ROWS
    total = parts[0:n, :].astype(F32)
    for y in range(1, NY):
        total = total + parts[n * y : n * (y + 1), :].astype(F32)
    slot = slot_of(gate_rows[...])
    a = lax.broadcasted_iota(jnp.int32, (TOK * TOK, TOK), 0)
    b = lax.broadcasted_iota(jnp.int32, (TOK * TOK, TOK), 1)
    spread = dot(one_hot(lax.shift_right_logical(a, 5), b), slot.astype(BF16))
    chunk = lax.bitwise_and(lax.broadcasted_iota(jnp.int32, (TOK * TOK, LANES), 0), TOK - 1)
    key = (chunk.astype(F32) * 16.0 + spread)[:, 0:1]
    out[...] = dot(one_hot(key, chunk_and_slot(iota((1, n), 1))), total.astype(BF16)).astype(BF16)


def finish_body(parts, out, total):
    n = 2 * TOK
    value = parts[0:n, :].astype(F32)
    for z in range(1, NZ):
        value = value + parts[n * z : n * (z + 1), :].astype(F32)
    total[...] = value
    for c in range(NC):
        for j in range(HALF):
            at = (c * HALF + j) * LANES
            row = c * TOK + j
            out[:, at : at + LANES] = total[row : row + 1, :].astype(BF16)


def exchange(x, axes, members):
    rows = x.shape[0] // members
    y = lax.all_to_all(
        x.reshape(members, rows, x.shape[1]), axes, split_axis=0, concat_axis=0, tiled=True
    )
    return y.reshape(x.shape)


def swapped(x, axis):
    return lax.ppermute(x, axis, [(0, 1), (1, 0)])


def x_swapped(x, mask):
    return lax.ppermute(x, ("xh", "xl"), [(i, i ^ mask) for i in range(NX)])


def rows_at(start, size):
    return pl.ds(pl.multiple_of(start, size), size)


def core_body(place_ids, w_in, w_out, up, down):
    other = 1 - place_ids[0]
    up[...] = w_in[rows_at(other * 2 * WIDTH, 2 * WIDTH), :]
    down[...] = w_out[:, rows_at(other * NX * WIDTH, NX * WIDTH)]


def up_row_body(place_ids, w_in, up, here, there):
    core, xh = place_ids[0], place_ids[1]
    for out, side in ((here, xh), (there, 1 - xh)):
        out[0:WIDTH, :] = w_in[rows_at((2 * core + side) * WIDTH, WIDTH), :]
        out[WIDTH : 2 * WIDTH, :] = up[rows_at(side * WIDTH, WIDTH), :]


def down_row_body(place_ids, w_out, down, *outs):
    core, x = place_ids[0], place_ids[2]
    for d, out in enumerate(outs):
        to = lax.bitwise_xor(x, jnp.int32(d))
        out[0:BLOCK, :] = w_out[:, rows_at((core * NX + to) * WIDTH, WIDTH)]
        out[BLOCK : 2 * BLOCK, :] = down[:, rows_at(to * WIDTH, WIDTH)]


def spread_weights(place_ids, w_in, w_out):
    shape = jax.ShapeDtypeStruct
    up_shape, down_shape = shape((2 * WIDTH, 2 * LANES), BF16), shape((2 * BLOCK, WIDTH), BF16)
    up, down = call(
        core_body,
        (up_shape, shape((BLOCK, NX * WIDTH), BF16)),
        (place_ids, w_in, w_out),
        smem=(0,),
    )
    up = swapped(up, "c")
    down = swapped(down, "c")
    up_here, up_there = call(
        up_row_body, (up_shape,) * 2, (place_ids, w_in, up), smem=(0,)
    )
    up_there = swapped(up_there, "xh")
    parts = call(
        down_row_body, (down_shape,) * NX, (place_ids, w_out, down), smem=(0,)
    )
    parts = list(parts)
    for d in range(1, NX):
        parts[d] = x_swapped(parts[d], d)
    return (up_here, up_there), parts


def layer(tokens, node_ids, gates, w_in, w_out):
    shape = jax.ShapeDtypeStruct
    core, xh, xl = (lax.axis_index(a).astype(jnp.int32) for a in ROW)
    place_ids = jnp.stack([core, xh, xh * NXL + xl])

    sent = call(
        spread_body,
        shape((TOK * TOK, LANES), BF16),
        (node_ids[0], gates[0], tokens[0]),
        scratch=(
            pltpu.VMEM((1, 4), jnp.int32),
            pltpu.VMEM((1, 8), BF16),
            pltpu.VMEM((1, 2 * HALF * LANES), BF16),
            pltpu.VMEM((2 * TOK, LANES), F32),
            pltpu.SemaphoreType.DMA((3,)),
        ),
        far=True,
    )
    sent, w_in, w_out = lax.optimization_barrier((sent, w_in, w_out))
    arrived = exchange(sent, COLUMN, NZ * NC)
    w_up, w_down = spread_weights(place_ids, w_in.reshape(4 * WIDTH, 2 * LANES), w_out[0])

    packed, gate_rows = call(
        pack_body,
        (shape((NY * NX * BLOCK_ROWS, LANES), BF16), shape((TOK, LANES), F32)),
        (arrived,),
    )
    rows = exchange(packed, PLANE, NY * NX)

    partial_sums, gate, balance = call(
        up_body,
        (shape((8 * ROWS, LANES), BF16), shape((ROWS, LANES), F32), shape((1,), F32)),
        (place_ids, rows, *w_up),
        scratch=(pltpu.VMEM((EIGHTH + 1, ROWS, LANES), F32),),
        smem=(0,),
        smem_out=(2,),
        flops=10**9,
    )
    summands = exchange(partial_sums, ROW, 8)

    hidden = call(hidden_body, shape((4 * ROWS, LANES), BF16), (summands, gate))
    every_hidden = exchange(hidden, ROW, 8)

    down = call(
        down_body,
        shape((NY * NX * BLOCK_ROWS, LANES), BF16),
        (place_ids, every_hidden, *w_down),
        scratch=(pltpu.VMEM((ROWS, WIDTH), F32),),
        smem=(0,),
        flops=10**9,
    )
    returned = exchange(down, PLANE, NY * NX)

    unpacked = call(
        unpack_body,
        shape((TOK * TOK, LANES), BF16),
        (returned, gate_rows),
    )
    back = exchange(unpacked, COLUMN, NZ * NC)

    mixed = call(
        finish_body,
        shape((1, 2 * HALF * LANES), BF16),
        (back,),
        scratch=(pltpu.VMEM((2 * TOK, LANES), F32),),
    )
    return mixed[None], balance


def solution(mesh):
    fine = Mesh(mesh.devices.reshape(NZ, NC, NY, NXH, NXL), AXES)
    token_spec = P(PLANE, COLUMN, None)
    return jax.shard_map(
        layer,
        mesh=fine,
        in_specs=(
            token_spec,
            token_spec,
            token_spec,
            P(AXES, None, None),
            P(COLUMN, PLANE, None),
        ),
        out_specs=(token_spec, P(COLUMN)),
        check_vma=False,
    )
```

```python
import jax
import jax.numpy as jnp
from jax import lax
from jax.experimental import pallas as pl
from jax.experimental.pallas import tpu as pltpu
from jax.sharding import Mesh
from jax.sharding import PartitionSpec as P


F32 = jnp.float32
BF16 = jnp.bfloat16

NZ, NC, NYH, NYL, NXH, NXL = 16, 2, 4, 2, 2, 2
COLUMNS = NYH * NYL * NXH * NXL
NQ = NYL * NXL
AXES = ("z", "c", "yh", "yl", "xh", "xl")
COLUMN = ("z", "c")
PLANE = ("yh", "yl", "xh", "xl")
QUAD = ("yl", "xl")
TEAM = ("c", "yl", "xl")


LANES = 128
SLOTS = 9
EIGHTH = 7
HALF = NQ * EIGHTH
TOK = 32
BLOCK_ROWS = 64
ROWS = COLUMNS * SLOTS
PAIR = ROWS // 4
BLOCK = 64
WIDTH = EIGHTH * LANES


def swap_halves(v):
    return pltpu.roll(v, LANES // 2, 1)


def left_half(shape):
    return lax.broadcasted_iota(jnp.int32, shape, 1) < LANES // 2


def one_hot(row_key, col_key):
    return (row_key == col_key).astype(F32).astype(BF16)


def iota(shape, axis):
    return lax.broadcasted_iota(jnp.int32, shape, axis).astype(F32)


def divided(value, by):
    quotient = jnp.floor((value + 0.5) * (1.0 / by))
    return quotient, value - by * quotient


def dot(a, b):
    return jnp.dot(a, b, preferred_element_type=F32)


def dot_t(a, b):
    return lax.dot_general(a, b, (((1,), (1,)), ((), ())), preferred_element_type=F32)


def call(body, outs, ins, scratch=(), smem=(), smem_out=(), far=False, flops=10**8, limit=24 * 2**20):
    def spec(in_smem):
        return pl.BlockSpec(memory_space=pltpu.SMEM if in_smem else pltpu.VMEM)

    far_spec = pl.BlockSpec(memory_space=pltpu.HBM)

    if far:
        ins = [pltpu.with_memory_space_constraint(x, pltpu.HBM) for x in ins]
    several = isinstance(outs, tuple)
    return pl.pallas_call(
        body,
        out_shape=outs,
        in_specs=[far_spec if far else spec(i in smem) for i in range(len(ins))],
        out_specs=tuple(spec(i in smem_out) for i in range(len(outs))) if several else spec(False),
        scratch_shapes=list(scratch),
        compiler_params=pltpu.CompilerParams(vmem_limit_bytes=limit),
        cost_estimate=pl.CostEstimate(flops=flops, bytes_accessed=10**6, transcendentals=0),
    )(*ins)


def spread_body(far_ids, far_gates, far_token, out, ids, gates, token, base, arrived):
    copies = [
        pltpu.make_async_copy(far, near, arrived.at[i])
        for i, (far, near) in enumerate(((far_token, token), (far_ids, ids), (far_gates, gates)))
    ]
    for copy in copies:
        copy.start()
    for copy in copies:
        copy.wait()
    for c in range(NC):
        for yl in range(NYL):
            for xl in range(NXL):
                for k in range(EIGHTH):
                    row = c * TOK + (yl * NXL + xl) * EIGHTH + k
                    i = xl * HALF + (c * NYL + yl) * EIGHTH + k
                    base[row : row + 1, :] = token[:, i * LANES : (i + 1) * LANES].astype(F32)
        base[c * TOK + HALF : (c + 1) * TOK, :] = jnp.zeros((TOK - HALF, LANES), F32)
    tile = (8, LANES)
    left = left_half(tile)
    gate_row = lax.broadcasted_iota(jnp.int32, tile, 0) == HALF % 8
    every_gate = gates[...].astype(F32)
    nodes, pairs = [], []
    for m in range(4):
        nodes.append(jnp.broadcast_to(ids[:, m : m + 1], tile))
        first = jnp.broadcast_to(every_gate[:, 2 * m : 2 * m + 1], tile)
        second = jnp.broadcast_to(every_gate[:, 2 * m + 1 : 2 * m + 2], tile)
        pairs.append(jnp.where(left, first, second))
    blocks = [base[8 * b : 8 * (b + 1), :] for b in range(2 * TOK // 8)]
    for z in range(NZ):
        gate = jnp.zeros(tile, F32)
        for node, pair in zip(nodes, pairs):
            gate = jnp.where(node == z, pair, gate)
        live = gate > 0
        rows = [jnp.where(live, block, 0.0) for block in blocks]
        for b in (HALF // 8, (TOK + HALF) // 8):
            rows[b] = jnp.where(gate_row, gate, rows[b])
        out[2 * TOK * z : 2 * TOK * (z + 1), :] = jnp.concatenate(rows, axis=0).astype(BF16)


def slot_of(gate_rows):
    live = (gate_rows > 0).astype(F32)
    a = lax.broadcasted_iota(jnp.int32, (TOK, TOK), 0)
    b = lax.broadcasted_iota(jnp.int32, (TOK, TOK), 1)
    order = dot((b <= a).astype(F32).astype(BF16), live.astype(BF16)) - 1.0
    return jnp.where(live > 0, order, 15.0)


def chunk_and_slot(at):
    x, row = divided(at, BLOCK_ROWS)
    k, r = divided(row, SLOTS)
    return jnp.where(k < EIGHTH, (x * EIGHTH + k) * 16.0 + r, -1.0)


def pack_body(arrived, out, gate_out):
    a = lax.broadcasted_iota(jnp.int32, (TOK, TOK * TOK), 0)
    b = lax.broadcasted_iota(jnp.int32, (TOK, TOK * TOK), 1)
    gate_rows = dot(one_hot(a * TOK + HALF, b), arrived[...])
    gate_out[...] = gate_rows
    slot = slot_of(gate_rows)
    lane = lax.broadcasted_iota(jnp.int32, (8, LANES), 1)
    by_token = dot_t(one_hot(lane, 0), slot.astype(BF16))
    token_of = lax.shift_right_logical(b, 5)
    spread = dot(by_token.astype(BF16), one_hot(a, token_of))
    chunk = lax.bitwise_and(b[0:1], TOK - 1).astype(F32)
    col_key = chunk * 16.0 + spread[0:1]
    row_key = chunk_and_slot(iota((NQ * BLOCK_ROWS, 1), 0))
    packed = dot(one_hot(row_key, col_key), arrived[...])
    lane = lax.broadcasted_iota(jnp.int32, (TOK, LANES), 1)
    wanted = lax.bitwise_and(lane, 15).astype(F32) == slot
    value = jnp.where(lane < 16, gate_rows, jnp.where(lane < 32, swap_halves(gate_rows), 0.0))
    gate_line = jnp.sum(jnp.where(wanted, value, 0.0), axis=0, keepdims=True)
    row = lax.broadcasted_iota(jnp.int32, packed.shape, 0)
    last = lax.bitwise_and(row, BLOCK_ROWS - 1) == BLOCK_ROWS - 1
    packed = jnp.where(last, gate_line, packed).astype(BF16)
    for t in range(COLUMNS):
        v = t // (NXH * NXL) % NYL * NXL + t % NXL
        out[t * BLOCK_ROWS : (t + 1) * BLOCK_ROWS, :] = packed[v * BLOCK_ROWS : (v + 1) * BLOCK_ROWS]


def up_body(place_ids, rows, w_here, w_there, out, gate_out, balance_out, x):
    core, yl = place_ids[0], place_ids[1]
    n = COLUMNS // 4 * BLOCK_ROWS
    column, row = divided(iota((1, n), 1), BLOCK_ROWS)
    k, r = divided(row, SLOTS)
    of_pair, _ = divided(iota((PAIR, 1), 0), SLOTS)
    p = jnp.concatenate(
        [
            one_hot(iota((EIGHTH * PAIR, n), 0), k * PAIR + column * SLOTS + r),
            one_hot((of_pair + 1.0) * BLOCK_ROWS - 1.0, iota((PAIR, n), 1)),
        ],
        axis=0,
    )
    for g in range(4):
        moved = dot(p, rows[n * g : n * (g + 1), :])
        for k in range(EIGHTH + 1):
            x[k, PAIR * g : PAIR * (g + 1), :] = moved[PAIR * k : PAIR * (k + 1), :]
    _, slot = divided(iota((ROWS, 1), 0), SLOTS)
    wanted = iota((ROWS, LANES), 1) == slot + 16.0 * core.astype(F32)
    gate = jnp.sum(jnp.where(wanted, x[EIGHTH], 0.0), axis=1, keepdims=True)
    gate_out[...] = jnp.broadcast_to(gate, (ROWS, LANES))
    scale = jnp.float32(1.0 / 256.0)
    count, total = jnp.sum((gate > 0).astype(F32)), jnp.sum(gate)
    balance_out[0] = (count * scale) * (total * scale)
    features = jnp.concatenate([x[k].astype(BF16) for k in range(EIGHTH)], axis=1)
    left = left_half((ROWS, LANES))
    for j in range(4):
        w = (w_here, w_there)[j // 2]
        both = dot(features, w[WIDTH * (j % 2) : WIDTH * (j % 2 + 1), :])
        g, u = both[:, :LANES], both[:, LANES:]
        expert = core if j % 2 == 0 else 1 - core
        part = yl if j < 2 else 1 - yl
        at = ROWS * 2 * (expert * NYL + part)
        out[pl.ds(pl.multiple_of(at, ROWS), ROWS), :] = jnp.where(left, g, swap_halves(u)).astype(BF16)
        at = at + ROWS
        out[pl.ds(pl.multiple_of(at, ROWS), ROWS), :] = jnp.where(left, swap_halves(g), u).astype(BF16)


def hidden_body(parts, gate, out):
    total = parts[0:ROWS, :].astype(F32)
    for j in range(1, 8):
        total = total + parts[ROWS * j : ROWS * (j + 1), :].astype(F32)
    up = swap_halves(total)
    h = gate[...] * (total / (1.0 + jnp.exp(-total))) * up
    half = ROWS // 2
    h = jnp.where(left_half((half, LANES)), h[:half], swap_halves(h[half:])).astype(BF16)
    for j in range(8):
        out[half * j : half * (j + 1), :] = h


def down_body(place_ids, hidden, w0, w1, w2, w3, out, acc):
    core, quad = place_ids[0], place_ids[2]
    half = ROWS // 2
    left = left_half((half, LANES))

    def block(expert, source):
        at = pl.multiple_of((expert * NQ + source) * half, half)
        return hidden[pl.ds(at, half), :].astype(F32)

    for d, w in enumerate((w0, w1, w2, w3)):
        source = lax.bitwise_xor(quad, jnp.int32(d))
        a, b = block(core, source), block(1 - core, source)
        top = dot(jnp.where(left, a, swap_halves(b)).astype(BF16), w[...])
        bottom = dot(jnp.where(left, swap_halves(a), b).astype(BF16), w[...])
        if d == 0:
            acc[0:half, :] = top
            acc[half:ROWS, :] = bottom
        else:
            acc[0:half, :] += top
            acc[half:ROWS, :] += bottom
    n = COLUMNS // 4 * BLOCK_ROWS
    k, row = divided(iota((1, EIGHTH * PAIR), 1), PAIR)
    column, r = divided(row, SLOTS)
    q = one_hot(iota((n, EIGHTH * PAIR), 0), column * BLOCK_ROWS + k * SLOTS + r)
    for g in range(4):
        stacked = jnp.concatenate(
            [acc[PAIR * g : PAIR * (g + 1), LANES * k : LANES * (k + 1)] for k in range(EIGHTH)],
            axis=0,
        ).astype(BF16)
        out[n * g : n * (g + 1), :] = dot(q, stacked).astype(BF16)


def unpack_body(parts, gate_rows, out):
    n = NQ * BLOCK_ROWS
    blocks = []
    for yl in range(NYL):
        for xl in range(NXL):
            block = jnp.zeros((BLOCK_ROWS, LANES), F32)
            for yh in range(NYH):
                for xh in range(NXH):
                    t = ((yh * NYL + yl) * NXH + xh) * NXL + xl
                    block = block + parts[t * BLOCK_ROWS : (t + 1) * BLOCK_ROWS, :].astype(F32)
            blocks.append(block)
    total = jnp.concatenate(blocks, axis=0)
    slot = slot_of(gate_rows[...])
    a = lax.broadcasted_iota(jnp.int32, (TOK * TOK, TOK), 0)
    b = lax.broadcasted_iota(jnp.int32, (TOK * TOK, TOK), 1)
    spread = dot(one_hot(lax.shift_right_logical(a, 5), b), slot.astype(BF16))
    chunk = lax.bitwise_and(lax.broadcasted_iota(jnp.int32, (TOK * TOK, LANES), 0), TOK - 1)
    key = (chunk.astype(F32) * 16.0 + spread)[:, 0:1]
    out[...] = dot(one_hot(key, chunk_and_slot(iota((1, n), 1))), total.astype(BF16)).astype(BF16)


def finish_body(parts, out, total):
    n = 2 * TOK
    value = parts[0:n, :].astype(F32)
    for z in range(1, NZ):
        value = value + parts[n * z : n * (z + 1), :].astype(F32)
    total[...] = value
    for c in range(NC):
        for j in range(HALF):
            at = (c * HALF + j) * LANES
            row = c * TOK + j
            out[:, at : at + LANES] = total[row : row + 1, :].astype(BF16)


def exchange(x, axes, members):
    rows = x.shape[0] // members
    y = lax.all_to_all(
        x.reshape(members, rows, x.shape[1]), axes, split_axis=0, concat_axis=0, tiled=True
    )
    return y.reshape(x.shape)


def swapped(x, axis):
    return lax.ppermute(x, axis, [(0, 1), (1, 0)])


def quad_swapped(x, mask):
    return lax.ppermute(x, QUAD, [(i, i ^ mask) for i in range(NQ)])


def rows_at(start, size):
    return pl.ds(pl.multiple_of(start, size), size)


def up_core_body(place_ids, w_in, up):
    up[...] = w_in[rows_at((1 - place_ids[0]) * 2 * WIDTH, 2 * WIDTH), :]


def down_core_body(place_ids, w_out, down):
    down[...] = w_out[:, rows_at((1 - place_ids[0]) * NQ * WIDTH, NQ * WIDTH)]


def up_quad_body(place_ids, w_in, up, here, there):
    core, yl = place_ids[0], place_ids[1]
    for out, side in ((here, yl), (there, 1 - yl)):
        out[0:WIDTH, :] = w_in[rows_at((2 * core + side) * WIDTH, WIDTH), :]
        out[WIDTH : 2 * WIDTH, :] = up[rows_at(side * WIDTH, WIDTH), :]


def down_quad_body(place_ids, w_out, down, *outs):
    core, quad = place_ids[0], place_ids[2]
    for d, out in enumerate(outs):
        to = lax.bitwise_xor(quad, jnp.int32(d))
        out[0:BLOCK, :] = w_out[:, rows_at((core * NQ + to) * WIDTH, WIDTH)]
        out[BLOCK : 2 * BLOCK, :] = down[:, rows_at(to * WIDTH, WIDTH)]


def spread_weights(place_ids, w_in, w_out):
    shape = jax.ShapeDtypeStruct
    up_shape, down_shape = shape((2 * WIDTH, 2 * LANES), BF16), shape((2 * BLOCK, WIDTH), BF16)
    up = call(up_core_body, up_shape, (place_ids, w_in), smem=(0,))
    up = swapped(up, "c")
    up_here, up_there = call(
        up_quad_body, (up_shape,) * 2, (place_ids, w_in, up), smem=(0,)
    )
    up_there = swapped(up_there, "yl")
    down = call(
        down_core_body, shape((BLOCK, NQ * WIDTH), BF16), (place_ids, w_out), smem=(0,)
    )
    down = swapped(down, "c")
    parts = call(
        down_quad_body, (down_shape,) * NQ, (place_ids, w_out, down), smem=(0,)
    )
    parts = list(parts)
    for d in range(1, NQ):
        parts[d] = quad_swapped(parts[d], d)
    return (up_here, up_there), parts


def layer(tokens, node_ids, gates, w_in, w_out):
    shape = jax.ShapeDtypeStruct
    core, yl, xl = (lax.axis_index(a).astype(jnp.int32) for a in TEAM)
    place_ids = jnp.stack([core, yl, yl * NXL + xl])

    sent = call(
        spread_body,
        shape((TOK * TOK, LANES), BF16),
        (node_ids[0], gates[0], tokens[0]),
        scratch=(
            pltpu.VMEM((1, 4), jnp.int32),
            pltpu.VMEM((1, 8), BF16),
            pltpu.VMEM((1, 2 * HALF * LANES), BF16),
            pltpu.VMEM((2 * TOK, LANES), F32),
            pltpu.SemaphoreType.DMA((3,)),
        ),
        far=True,
    )
    sent, w_in, w_out = lax.optimization_barrier((sent, w_in, w_out))
    arrived = exchange(sent, COLUMN, NZ * NC)
    w_up, w_down = spread_weights(place_ids, w_in.reshape(4 * WIDTH, 2 * LANES), w_out[0])

    packed, gate_rows = call(
        pack_body,
        (shape((COLUMNS * BLOCK_ROWS, LANES), BF16), shape((TOK, LANES), F32)),
        (arrived,),
    )
    rows = exchange(packed, PLANE, COLUMNS)

    partial_sums, gate, balance = call(
        up_body,
        (shape((8 * ROWS, LANES), BF16), shape((ROWS, LANES), F32), shape((1,), F32)),
        (place_ids, rows, *w_up),
        scratch=(pltpu.VMEM((EIGHTH + 1, ROWS, LANES), F32),),
        smem=(0,),
        smem_out=(2,),
        flops=10**9,
    )
    summands = exchange(partial_sums, TEAM, 8)

    hidden = call(hidden_body, shape((4 * ROWS, LANES), BF16), (summands, gate))
    every_hidden = exchange(hidden, TEAM, 8)

    down = call(
        down_body,
        shape((COLUMNS * BLOCK_ROWS, LANES), BF16),
        (place_ids, every_hidden, *w_down),
        scratch=(pltpu.VMEM((ROWS, WIDTH), F32),),
        smem=(0,),
        flops=10**9,
    )
    returned = exchange(down, PLANE, COLUMNS)

    unpacked = call(
        unpack_body,
        shape((TOK * TOK, LANES), BF16),
        (returned, gate_rows),
    )
    back = exchange(unpacked, COLUMN, NZ * NC)

    mixed = call(
        finish_body,
        shape((1, 2 * HALF * LANES), BF16),
        (back,),
        scratch=(pltpu.VMEM((2 * TOK, LANES), F32),),
    )
    return mixed[None], balance


def solution(mesh):
    fine = Mesh(mesh.devices.reshape(NZ, NC, NYH, NYL, NXH, NXL), AXES)
    token_spec = P(PLANE, COLUMN, None)
    return jax.shard_map(
        layer,
        mesh=fine,
        in_specs=(
            token_spec,
            token_spec,
            token_spec,
            P(AXES, None, None),
            P(COLUMN, PLANE, None),
        ),
        out_specs=(token_spec, P(COLUMN)),
        check_vma=False,
    )
```

```python
import jax
import jax.numpy as jnp
from jax import lax
from jax.experimental import pallas as pl
from jax.experimental.pallas import tpu as pltpu
from jax.sharding import Mesh
from jax.sharding import PartitionSpec as P


F32 = jnp.float32
BF16 = jnp.bfloat16

NZ, NC, NY, NXH, NXL = 16, 2, 8, 2, 2
NX = NXH * NXL
AXES = ("z", "c", "y", "xh", "xl")
COLUMN = ("z", "c")
PLANE = ("y", "xh", "xl")
ROW = ("c", "xh", "xl")

FIRST_PLANE_IN, FIRST_PLANE_OUT = 10, 8
FIRST_COLUMN_IN, FIRST_COLUMN_OUT = 16, 16

LANES = 128
SLOTS = 9
EIGHTH = 7
HALF = NX * EIGHTH
TOK = 32
BLOCK_ROWS = 64
ROWS = NY * NX * SLOTS
PAIR = ROWS // 4
BLOCK = 64
WIDTH = EIGHTH * LANES


def swap_halves(v):
    return pltpu.roll(v, LANES // 2, 1)


def left_half(shape):
    return lax.broadcasted_iota(jnp.int32, shape, 1) < LANES // 2


def one_hot(row_key, col_key):
    return (row_key == col_key).astype(F32).astype(BF16)


def iota(shape, axis):
    return lax.broadcasted_iota(jnp.int32, shape, axis).astype(F32)


def divided(value, by):
    quotient = jnp.floor((value + 0.5) * (1.0 / by))
    return quotient, value - by * quotient


def rows_at(start, size):
    return pl.ds(pl.multiple_of(start, size), size)


def dot(a, b):
    return jnp.dot(a, b, preferred_element_type=F32)


def dot_t(a, b):
    return lax.dot_general(a, b, (((1,), (1,)), ((), ())), preferred_element_type=F32)


def call(body, outs, ins, scratch=(), smem=(), smem_out=(), far=(), flops=10**8, limit=24 * 2**20):
    def spec(in_smem):
        return pl.BlockSpec(memory_space=pltpu.SMEM if in_smem else pltpu.VMEM)

    far_spec = pl.BlockSpec(memory_space=pltpu.HBM)

    ins = [pltpu.with_memory_space_constraint(x, pltpu.HBM) if i in far else x for i, x in enumerate(ins)]
    several = isinstance(outs, tuple)
    return pl.pallas_call(
        body,
        out_shape=outs,
        in_specs=[far_spec if i in far else spec(i in smem) for i in range(len(ins))],
        out_specs=tuple(spec(i in smem_out) for i in range(len(outs))) if several else spec(False),
        scratch_shapes=list(scratch),
        compiler_params=pltpu.CompilerParams(vmem_limit_bytes=limit),
        cost_estimate=pl.CostEstimate(flops=flops, bytes_accessed=10**6, transcendentals=0),
    )(*ins)


def spread_body(far_ids, far_gates, far_token, out, ids, gates, token, base, arrived):
    copies = [
        pltpu.make_async_copy(far, near, arrived.at[i])
        for i, (far, near) in enumerate(((far_token, token), (far_ids, ids), (far_gates, gates)))
    ]
    for copy in copies:
        copy.start()
    for copy in copies:
        copy.wait()
    for c in range(NC):
        for xh in range(NXH):
            for xl in range(NXL):
                for k in range(EIGHTH):
                    row = c * TOK + (xh * NXL + xl) * EIGHTH + k
                    i = xl * HALF + (c * NXH + xh) * EIGHTH + k
                    base[row : row + 1, :] = token[:, i * LANES : (i + 1) * LANES].astype(F32)
        base[c * TOK + HALF : (c + 1) * TOK, :] = jnp.zeros((TOK - HALF, LANES), F32)
    tile = (8, LANES)
    left = left_half(tile)
    gate_row = lax.broadcasted_iota(jnp.int32, tile, 0) == HALF % 8
    every_gate = gates[...].astype(F32)
    nodes, pairs = [], []
    for m in range(4):
        nodes.append(jnp.broadcast_to(ids[:, m : m + 1], tile))
        first = jnp.broadcast_to(every_gate[:, 2 * m : 2 * m + 1], tile)
        second = jnp.broadcast_to(every_gate[:, 2 * m + 1 : 2 * m + 2], tile)
        pairs.append(jnp.where(left, first, second))
    blocks = [base[8 * b : 8 * (b + 1), :] for b in range(2 * TOK // 8)]
    for z in range(NZ):
        gate = jnp.zeros(tile, F32)
        for node, pair in zip(nodes, pairs):
            gate = jnp.where(node == (z + FIRST_PLANE_IN) % NZ, pair, gate)
        live = gate > 0
        rows = [jnp.where(live, block, 0.0) for block in blocks]
        for b in (HALF // 8, (TOK + HALF) // 8):
            rows[b] = jnp.where(gate_row, gate, rows[b])
        out[2 * TOK * z : 2 * TOK * (z + 1), :] = jnp.concatenate(rows, axis=0).astype(BF16)


def slot_of(gate_rows):
    live = (gate_rows > 0).astype(F32)
    a = lax.broadcasted_iota(jnp.int32, (TOK, TOK), 0)
    b = lax.broadcasted_iota(jnp.int32, (TOK, TOK), 1)
    order = dot((b <= a).astype(F32).astype(BF16), live.astype(BF16)) - 1.0
    return jnp.where(live > 0, order, 15.0)


def chunk_and_slot(at):
    x, row = divided(at, BLOCK_ROWS)
    k, r = divided(row, SLOTS)
    return jnp.where(k < EIGHTH, (x * EIGHTH + k) * 16.0 + r, -1.0)


def pack_body(arrived, out, gate_out):
    a = lax.broadcasted_iota(jnp.int32, (TOK, TOK * TOK), 0)
    b = lax.broadcasted_iota(jnp.int32, (TOK, TOK * TOK), 1)
    gate_rows = dot(one_hot(a * TOK + HALF, b), arrived[...])
    gate_out[...] = gate_rows
    slot = slot_of(gate_rows)
    lane = lax.broadcasted_iota(jnp.int32, (8, LANES), 1)
    by_token = dot_t(one_hot(lane, 0), slot.astype(BF16))
    token_of = lax.shift_right_logical(b, 5)
    spread = dot(by_token.astype(BF16), one_hot(a, token_of))
    chunk = lax.bitwise_and(b[0:1], TOK - 1).astype(F32)
    col_key = chunk * 16.0 + spread[0:1]
    row_key = chunk_and_slot(iota((NX * BLOCK_ROWS, 1), 0))
    packed = dot(one_hot(row_key, col_key), arrived[...])
    lane = lax.broadcasted_iota(jnp.int32, (TOK, LANES), 1)
    wanted = lax.bitwise_and(lane, 15).astype(F32) == slot
    value = jnp.where(lane < 16, gate_rows, jnp.where(lane < 32, swap_halves(gate_rows), 0.0))
    gate_line = jnp.sum(jnp.where(wanted, value, 0.0), axis=0, keepdims=True)
    row = lax.broadcasted_iota(jnp.int32, packed.shape, 0)
    last = lax.bitwise_and(row, BLOCK_ROWS - 1) == BLOCK_ROWS - 1
    packed = jnp.where(last, gate_line, packed).astype(BF16)
    for y in range(NY):
        out[y * NX * BLOCK_ROWS : (y + 1) * NX * BLOCK_ROWS, :] = packed


def up_body(place_ids, far_w, rows, w_core, w_row, w_both, out, gate_out, balance_out, x, w_own, done):
    core, xh = place_ids[0], place_ids[1]
    own = pltpu.make_async_copy(far_w.at[rows_at((2 * core + xh) * WIDTH, WIDTH)], w_own, done.at[0])
    own.start()
    n = 2 * NX * BLOCK_ROWS
    column, row = divided(iota((1, n), 1), BLOCK_ROWS)
    k, r = divided(row, SLOTS)
    of_pair, _ = divided(iota((PAIR, 1), 0), SLOTS)
    p = jnp.concatenate(
        [
            one_hot(iota((EIGHTH * PAIR, n), 0), k * PAIR + column * SLOTS + r),
            one_hot((of_pair + 1.0) * BLOCK_ROWS - 1.0, iota((PAIR, n), 1)),
        ],
        axis=0,
    )
    for g in range(4):
        moved = dot(p, rows[n * g : n * (g + 1), :])
        for k in range(EIGHTH + 1):
            x[k, PAIR * g : PAIR * (g + 1), :] = moved[PAIR * k : PAIR * (k + 1), :]
    _, slot = divided(iota((ROWS, 1), 0), SLOTS)
    wanted = iota((ROWS, LANES), 1) == slot + 16.0 * core.astype(F32)
    gate = jnp.sum(jnp.where(wanted, x[EIGHTH], 0.0), axis=1, keepdims=True)
    gate_out[...] = jnp.broadcast_to(gate, (ROWS, LANES))
    scale = jnp.float32(1.0 / 256.0)
    count, total = jnp.sum((gate > 0).astype(F32)), jnp.sum(gate)
    balance_out[0] = (count * scale) * (total * scale)
    features = jnp.concatenate([x[k].astype(BF16) for k in range(EIGHTH)], axis=1)
    left = left_half((ROWS, LANES))
    for w, other_core, other_row in (
        (w_core, True, False),
        (w_row, False, True),
        (w_both, True, True),
        (w_own, False, False),
    ):
        if w is w_own:
            own.wait()
        both = dot(features, w[...])
        g, u = both[:, :LANES], both[:, LANES:]
        expert = 1 - core if other_core else core
        part = 1 - xh if other_row else xh
        at = ROWS * 2 * (expert * NXH + part)
        out[rows_at(at, ROWS), :] = jnp.where(left, g, swap_halves(u)).astype(BF16)
        out[rows_at(at + ROWS, ROWS), :] = jnp.where(left, swap_halves(g), u).astype(BF16)


def hidden_body(parts, gate, out):
    total = parts[0:ROWS, :].astype(F32)
    for j in range(1, 8):
        total = total + parts[ROWS * j : ROWS * (j + 1), :].astype(F32)
    up = swap_halves(total)
    h = gate[...] * (total / (1.0 + jnp.exp(-total))) * up
    half = ROWS // 2
    h = jnp.where(left_half((half, LANES)), h[:half], swap_halves(h[half:])).astype(BF16)
    for j in range(8):
        out[half * j : half * (j + 1), :] = h


def down_body(place_ids, hidden, w0, w1, w2, w3, out, acc):
    core, x = place_ids[0], place_ids[2]
    half = ROWS // 2
    left = left_half((half, LANES))

    def block(expert, source):
        at = pl.multiple_of((expert * NX + source) * half, half)
        return hidden[pl.ds(at, half), :].astype(F32)

    for d, w in enumerate((w0, w1, w2, w3)):
        source = lax.bitwise_xor(x, jnp.int32(d))
        a, b = block(core, source), block(1 - core, source)
        top = dot(jnp.where(left, a, swap_halves(b)).astype(BF16), w[...])
        bottom = dot(jnp.where(left, swap_halves(a), b).astype(BF16), w[...])
        if d == 0:
            acc[0:half, :] = top
            acc[half:ROWS, :] = bottom
        else:
            acc[0:half, :] += top
            acc[half:ROWS, :] += bottom
    n = 2 * NX * BLOCK_ROWS
    k, row = divided(iota((1, EIGHTH * PAIR), 1), PAIR)
    column, r = divided(row, SLOTS)
    q = one_hot(iota((n, EIGHTH * PAIR), 0), column * BLOCK_ROWS + k * SLOTS + r)
    for g in range(4):
        stacked = jnp.concatenate(
            [acc[PAIR * g : PAIR * (g + 1), LANES * k : LANES * (k + 1)] for k in range(EIGHTH)],
            axis=0,
        ).astype(BF16)
        out[n * g : n * (g + 1), :] = dot(q, stacked).astype(BF16)


def unpack_body(parts, gate_rows, out):
    n = NX * BLOCK_ROWS
    total = parts[0:n, :].astype(F32)
    for y in range(1, NY):
        total = total + parts[n * y : n * (y + 1), :].astype(F32)
    slot = slot_of(gate_rows[...])
    a = lax.broadcasted_iota(jnp.int32, (TOK * TOK, TOK), 0)
    b = lax.broadcasted_iota(jnp.int32, (TOK * TOK, TOK), 1)
    token = lax.shift_right_logical(a, 5) + NC * (FIRST_PLANE_OUT - FIRST_PLANE_IN)
    spread = dot(one_hot(lax.bitwise_and(token, TOK - 1), b), slot.astype(BF16))
    chunk = lax.bitwise_and(lax.broadcasted_iota(jnp.int32, (TOK * TOK, LANES), 0), TOK - 1)
    key = (chunk.astype(F32) * 16.0 + spread)[:, 0:1]
    out[...] = dot(one_hot(key, chunk_and_slot(iota((1, n), 1))), total.astype(BF16)).astype(BF16)


def finish_body(parts, out, total):
    n = 2 * TOK
    value = parts[0:n, :].astype(F32)
    for z in range(1, NZ):
        value = value + parts[n * z : n * (z + 1), :].astype(F32)
    total[...] = value
    for c in range(NC):
        for j in range(HALF):
            at = (c * HALF + j) * LANES
            row = c * TOK + j
            out[:, at : at + LANES] = total[row : row + 1, :].astype(BF16)


def exchange(x, axes, members, turn=0):
    rows = x.shape[0] // members
    order = [[(i + turn) % members for i in range(members)]] if turn else None
    y = lax.all_to_all(
        x.reshape(members, rows, x.shape[1]),
        axes,
        split_axis=0,
        concat_axis=0,
        axis_index_groups=order,
        tiled=True,
    )
    return y.reshape(x.shape)


def up_parts_body(place_ids, far_w, core_out, row_out, both_out, done):
    core, xh = place_ids[0], place_ids[1]
    to = (2 * (1 - core) + xh, 2 * core + 1 - xh, 2 * (1 - core) + 1 - xh)
    copies = [
        pltpu.make_async_copy(far_w.at[rows_at(eighth * WIDTH, WIDTH)], out, done.at[i])
        for i, (eighth, out) in enumerate(zip(to, (core_out, row_out, both_out)))
    ]
    for copy in copies:
        copy.start()
    for copy in copies:
        copy.wait()


def down_row_body(place_ids, w_out, other, *outs):
    core, x = place_ids[0], place_ids[2]
    for d, out in enumerate(outs):
        to = (core * NX + lax.bitwise_xor(x, jnp.int32(d))) * WIDTH
        out[0:BLOCK, :] = w_out[:, rows_at(to, WIDTH)]
        out[BLOCK : 2 * BLOCK, :] = other[:, rows_at(to, WIDTH)]


def up_weights(place_ids, w_in):
    parts = call(
        up_parts_body,
        (jax.ShapeDtypeStruct((WIDTH, 2 * LANES), BF16),) * 3,
        (place_ids, w_in),
        scratch=(pltpu.SemaphoreType.DMA((3,)),),
        smem=(0,),
        far=(1,),
    )
    swaps = ("c", [(0, 1), (1, 0)]), ("xh", [(0, 1), (1, 0)]), (("c", "xh"), [(i, 3 - i) for i in range(4)])
    out = []
    for i in (1, 2, 0):
        out.append(lax.ppermute(parts[i], *swaps[i]))
    return out[2], out[0], out[1]


def down_weights(place_ids, w_out):
    other = lax.ppermute(w_out, "c", [(0, 1), (1, 0)])
    parts = call(
        down_row_body,
        (jax.ShapeDtypeStruct((2 * BLOCK, WIDTH), BF16),) * NX,
        (place_ids, w_out, other),
        smem=(0,),
    )
    parts = list(parts)
    for d in range(1, NX):
        parts[d] = lax.ppermute(parts[d], ("xh", "xl"), [(i, i ^ d) for i in range(NX)])
    return parts


def layer(tokens, node_ids, gates, w_in, w_out):
    shape = jax.ShapeDtypeStruct
    core, xh, xl = (lax.axis_index(a).astype(jnp.int32) for a in ROW)
    place_ids = jnp.stack([core, xh, xh * NXL + xl])

    sent = call(
        spread_body,
        shape((TOK * TOK, LANES), BF16),
        (node_ids[0], gates[0], tokens[0]),
        scratch=(
            pltpu.VMEM((1, 4), jnp.int32),
            pltpu.VMEM((1, 8), BF16),
            pltpu.VMEM((1, 2 * HALF * LANES), BF16),
            pltpu.VMEM((2 * TOK, LANES), F32),
            pltpu.SemaphoreType.DMA((3,)),
        ),
        far=(0, 1, 2),
    )
    sent, w_in, w_out = lax.optimization_barrier((sent, w_in, w_out))
    arrived = exchange(sent, COLUMN, NZ * NC, NC * FIRST_PLANE_IN)
    w_in = w_in.reshape(4 * WIDTH, 2 * LANES)
    w_up = up_weights(place_ids, w_in)
    w_down = down_weights(place_ids, w_out[0])

    packed, gate_rows = call(
        pack_body,
        (shape((NY * NX * BLOCK_ROWS, LANES), BF16), shape((TOK, LANES), F32)),
        (arrived,),
    )
    rows = exchange(packed, PLANE, NY * NX, FIRST_COLUMN_IN)

    partial_sums, gate, balance = call(
        up_body,
        (shape((8 * ROWS, LANES), BF16), shape((ROWS, LANES), F32), shape((1,), F32)),
        (place_ids, w_in, rows, *w_up),
        scratch=(
            pltpu.VMEM((EIGHTH + 1, ROWS, LANES), F32),
            pltpu.VMEM((WIDTH, 2 * LANES), BF16),
            pltpu.SemaphoreType.DMA((1,)),
        ),
        smem=(0,),
        smem_out=(2,),
        far=(1,),
        flops=10**9,
    )
    summands = exchange(partial_sums, ROW, 8)

    hidden = call(hidden_body, shape((4 * ROWS, LANES), BF16), (summands, gate))
    every_hidden = exchange(hidden, ROW, 8)

    down = call(
        down_body,
        shape((NY * NX * BLOCK_ROWS, LANES), BF16),
        (place_ids, every_hidden, *w_down),
        scratch=(pltpu.VMEM((ROWS, WIDTH), F32),),
        smem=(0,),
        flops=10**9,
    )
    returned = exchange(down, PLANE, NY * NX, FIRST_COLUMN_OUT)

    unpacked = call(
        unpack_body,
        shape((TOK * TOK, LANES), BF16),
        (returned, gate_rows),
    )
    back = exchange(unpacked, COLUMN, NZ * NC, NC * FIRST_PLANE_OUT)

    mixed = call(
        finish_body,
        shape((1, 2 * HALF * LANES), BF16),
        (back,),
        scratch=(pltpu.VMEM((2 * TOK, LANES), F32),),
    )
    return mixed[None], balance


def solution(mesh):
    fine = Mesh(mesh.devices.reshape(NZ, NC, NY, NXH, NXL), AXES)
    token_spec = P(PLANE, COLUMN, None)
    return jax.shard_map(
        layer,
        mesh=fine,
        in_specs=(
            token_spec,
            token_spec,
            token_spec,
            P(AXES, None, None),
            P(COLUMN, PLANE, None),
        ),
        out_specs=(token_spec, P(COLUMN)),
        check_vma=False,
    )
```

```python
import jax
import jax.numpy as jnp
from jax import lax
from jax.experimental import pallas as pl
from jax.experimental.pallas import tpu as pltpu
from jax.sharding import Mesh
from jax.sharding import PartitionSpec as P


F32 = jnp.float32
BF16 = jnp.bfloat16

NZ, NC, NY, NXH, NXL = 16, 2, 8, 2, 2
NX = NXH * NXL
AXES = ("z", "c", "y", "xh", "xl")
COLUMN = ("z", "c")
PLANE = ("y", "xh", "xl")
ROW = ("c", "xh", "xl")

FIRST_PLANE_IN, FIRST_PLANE_OUT = 13, 8
FIRST_COLUMN = 18

LANES = 128
SLOTS = 9
EIGHTH = 7
HALF = NX * EIGHTH
TOK = 32
TOKEN_ROWS = 30
BLOCK_ROWS = 64
ROWS = NY * NX * SLOTS
PAIR = ROWS // 4
BLOCK = 64
WIDTH = EIGHTH * LANES


def swap_halves(v):
    return pltpu.roll(v, LANES // 2, 1)


def left_half(shape):
    return lax.broadcasted_iota(jnp.int32, shape, 1) < LANES // 2


def one_hot(row_key, col_key):
    return (row_key == col_key).astype(F32).astype(BF16)


def iota(shape, axis):
    return lax.broadcasted_iota(jnp.int32, shape, axis).astype(F32)


def divided(value, by):
    quotient = jnp.floor((value + 0.5) * (1.0 / by))
    return quotient, value - by * quotient


def rows_at(start, size):
    return pl.ds(pl.multiple_of(start, size), size)


def dot(a, b):
    return jnp.dot(a, b, preferred_element_type=F32)


def dot_t(a, b):
    return lax.dot_general(a, b, (((1,), (1,)), ((), ())), preferred_element_type=F32)


def call(body, outs, ins, scratch=(), smem=(), smem_out=(), far=(), flops=10**8, limit=24 * 2**20):
    def spec(in_smem):
        return pl.BlockSpec(memory_space=pltpu.SMEM if in_smem else pltpu.VMEM)

    far_spec = pl.BlockSpec(memory_space=pltpu.HBM)

    ins = [pltpu.with_memory_space_constraint(x, pltpu.HBM) if i in far else x for i, x in enumerate(ins)]
    several = isinstance(outs, tuple)
    return pl.pallas_call(
        body,
        out_shape=outs,
        in_specs=[far_spec if i in far else spec(i in smem) for i in range(len(ins))],
        out_specs=tuple(spec(i in smem_out) for i in range(len(outs))) if several else spec(False),
        scratch_shapes=list(scratch),
        compiler_params=pltpu.CompilerParams(vmem_limit_bytes=limit),
        cost_estimate=pl.CostEstimate(flops=flops, bytes_accessed=10**6, transcendentals=0),
    )(*ins)


def spread_body(far_ids, far_gates, far_token, out, ids, gates, token, base, arrived):
    copies = [
        pltpu.make_async_copy(far, near, arrived.at[i])
        for i, (far, near) in enumerate(((far_token, token), (far_ids, ids), (far_gates, gates)))
    ]
    for copy in copies:
        copy.start()
    for copy in copies:
        copy.wait()
    pair_rows = NC * TOKEN_ROWS
    base[...] = jnp.zeros(base.shape, F32)
    for c in range(NC):
        for xh in range(NXH):
            for xl in range(NXL):
                for k in range(EIGHTH):
                    row = c * TOKEN_ROWS + (xh * NXL + xl) * EIGHTH + k
                    i = xl * HALF + (c * NXH + xh) * EIGHTH + k
                    piece = token[:, i * LANES : (i + 1) * LANES].astype(F32)
                    base[row : row + 1, :] = piece
                    base[pair_rows + row : pair_rows + row + 1, :] = piece
    tile = (8, LANES)
    left = left_half(tile)
    sub = lax.broadcasted_iota(jnp.int32, tile, 0)
    every_gate = gates[...].astype(F32)
    nodes, pairs = [], []
    for m in range(4):
        nodes.append(jnp.broadcast_to(ids[:, m : m + 1], tile))
        first = jnp.broadcast_to(every_gate[:, 2 * m : 2 * m + 1], tile)
        second = jnp.broadcast_to(every_gate[:, 2 * m + 1 : 2 * m + 2], tile)
        pairs.append(jnp.where(left, first, second))

    def gate_of(place):
        gate = jnp.zeros(tile, F32)
        for node, pair in zip(nodes, pairs):
            gate = jnp.where(node == (place + FIRST_PLANE_IN) % NZ, pair, gate)
        return gate

    blocks = [base[8 * b : 8 * (b + 1), :] for b in range(2 * pair_rows // 8)]
    for z in range(0, NZ, 2):
        both = gate_of(z), gate_of(z + 1)
        rows = []
        for b, block in enumerate(blocks):
            split = min(max(pair_rows - 8 * b, 0), 8)
            gate = both[1] if split == 0 else both[0] if split == 8 else jnp.where(sub < split, *both)
            block = jnp.where(gate > 0, block, 0.0)
            for half in range(2 * NC):
                at = half * TOKEN_ROWS + HALF - 8 * b
                if 0 <= at < 8:
                    block = jnp.where(sub == at, gate, block)
            rows.append(block)
        out[pair_rows * z : pair_rows * (z + 2), :] = jnp.concatenate(rows, axis=0).astype(BF16)


def slot_of(gate_rows):
    live = (gate_rows > 0).astype(F32)
    a = lax.broadcasted_iota(jnp.int32, (TOK, TOK), 0)
    b = lax.broadcasted_iota(jnp.int32, (TOK, TOK), 1)
    order = dot((b <= a).astype(F32).astype(BF16), live.astype(BF16)) - 1.0
    return jnp.where(live > 0, order, 15.0)


def chunk_and_slot(at):
    x, row = divided(at, BLOCK_ROWS)
    x = jnp.where(x < NXL, x + NXL, x - NXL)
    k, r = divided(row, SLOTS)
    return jnp.where(k < EIGHTH, (x * EIGHTH + k) * 16.0 + r, -1.0)


def pack_body(arrived, out, gate_out):
    n = TOK * TOKEN_ROWS
    token, at = iota((TOK, n), 0), iota((1, n), 1)
    token_of, chunk = divided(at, TOKEN_ROWS)
    gate_rows = dot(one_hot(token * TOKEN_ROWS + HALF, at), arrived[...])
    gate_out[...] = gate_rows
    slot = slot_of(gate_rows)
    lane = lax.broadcasted_iota(jnp.int32, (8, LANES), 1)
    by_token = dot_t(one_hot(lane, 0), slot.astype(BF16))
    spread = dot(by_token.astype(BF16), one_hot(token, token_of))
    col_key = chunk * 16.0 + spread[0:1]
    row_key = chunk_and_slot(iota((NX * BLOCK_ROWS, 1), 0))
    packed = dot(one_hot(row_key, col_key), arrived[...])
    lane = lax.broadcasted_iota(jnp.int32, (TOK, LANES), 1)
    wanted = lax.bitwise_and(lane, 15).astype(F32) == slot
    value = jnp.where(lane < 16, gate_rows, jnp.where(lane < 32, swap_halves(gate_rows), 0.0))
    gate_line = jnp.sum(jnp.where(wanted, value, 0.0), axis=0, keepdims=True)
    row = lax.broadcasted_iota(jnp.int32, packed.shape, 0)
    last = lax.bitwise_and(row, BLOCK_ROWS - 1) == BLOCK_ROWS - 1
    packed = jnp.where(last, gate_line, packed).astype(BF16)
    for y in range(NY):
        out[y * NX * BLOCK_ROWS : (y + 1) * NX * BLOCK_ROWS, :] = packed


def up_body(place_ids, far_w, rows, w_core, w_row, w_both, out, gate_out, balance_out, x, w_own, done):
    core, xh = place_ids[0], place_ids[1]
    own = pltpu.make_async_copy(far_w.at[rows_at((2 * core + xh) * WIDTH, WIDTH)], w_own, done.at[0])
    own.start()
    n = 2 * NX * BLOCK_ROWS
    column, row = divided(iota((1, n), 1), BLOCK_ROWS)
    k, r = divided(row, SLOTS)
    of_pair, _ = divided(iota((PAIR, 1), 0), SLOTS)
    p = jnp.concatenate(
        [
            one_hot(iota((EIGHTH * PAIR, n), 0), k * PAIR + column * SLOTS + r),
            one_hot((of_pair + 1.0) * BLOCK_ROWS - 1.0, iota((PAIR, n), 1)),
        ],
        axis=0,
    )
    for g in range(0, 4, 2):
        moved = dot(p, jnp.concatenate([rows[n * (g + i) : n * (g + i + 1), :] for i in range(2)], axis=1))
        for i in range(2):
            at = PAIR * (g + i)
            for k in range(EIGHTH + 1):
                x[k, at : at + PAIR, :] = moved[PAIR * k : PAIR * (k + 1), LANES * i : LANES * (i + 1)]
    _, slot = divided(iota((ROWS, 1), 0), SLOTS)
    wanted = iota((ROWS, LANES), 1) == slot + 16.0 * core.astype(F32)
    gate = jnp.sum(jnp.where(wanted, x[EIGHTH], 0.0), axis=1, keepdims=True)
    gate_out[...] = jnp.broadcast_to(gate, (ROWS, LANES))
    scale = jnp.float32(1.0 / 256.0)
    count, total = jnp.sum((gate > 0).astype(F32)), jnp.sum(gate)
    balance_out[0] = (count * scale) * (total * scale)
    features = jnp.concatenate([x[k].astype(BF16) for k in range(EIGHTH)], axis=1)
    left = left_half((ROWS, LANES))
    for w, other_core, other_row in (
        (w_core, True, False),
        (w_row, False, True),
        (w_both, True, True),
        (w_own, False, False),
    ):
        if w is w_own:
            own.wait()
        both = dot(features, w[...])
        g, u = both[:, :LANES], both[:, LANES:]
        expert = 1 - core if other_core else core
        part = xh if other_row else 1 - xh
        at = ROWS * 2 * (expert * NXH + part)
        out[rows_at(at, ROWS), :] = jnp.where(left, g, swap_halves(u)).astype(BF16)
        out[rows_at(at + ROWS, ROWS), :] = jnp.where(left, swap_halves(g), u).astype(BF16)


def hidden_body(parts, gate, out):
    total = parts[0:ROWS, :].astype(F32)
    for j in range(1, 8):
        total = total + parts[ROWS * j : ROWS * (j + 1), :].astype(F32)
    up = swap_halves(total)
    h = gate[...] * (total / (1.0 + jnp.exp(-total))) * up
    half = ROWS // 2
    h = jnp.where(left_half((half, LANES)), h[:half], swap_halves(h[half:])).astype(BF16)
    for j in range(8):
        out[half * j : half * (j + 1), :] = h


def down_body(place_ids, hidden, w0, w1, w2, w3, out, acc):
    core, x = place_ids[0], place_ids[2]
    half = ROWS // 2
    left = left_half((half, LANES))

    def block(expert, source):
        return hidden[rows_at((expert * NX + source) * half, half), :].astype(F32)

    pairs = []
    for d in range(NX):
        source = lax.bitwise_xor(x, jnp.int32(d ^ 2))
        a, b = block(core, source), block(1 - core, source)
        top, bottom = jnp.where(left, a, swap_halves(b)), jnp.where(left, swap_halves(a), b)
        pairs.append(jnp.concatenate([top, bottom], axis=0).astype(BF16))
    w = jnp.concatenate([w0[...], w1[...], w2[...], w3[...]], axis=0)
    acc[...] = dot(jnp.concatenate(pairs, axis=1), w)
    n = 2 * NX * BLOCK_ROWS
    k, row = divided(iota((1, EIGHTH * PAIR), 1), PAIR)
    column, r = divided(row, SLOTS)
    q = one_hot(iota((n, EIGHTH * PAIR), 0), column * BLOCK_ROWS + k * SLOTS + r)

    def stacked(g):
        pieces = [acc[PAIR * g : PAIR * (g + 1), LANES * k : LANES * (k + 1)] for k in range(EIGHTH)]
        return jnp.concatenate(pieces, axis=0).astype(BF16)

    for g in range(0, 4, 2):
        both = dot(q, jnp.concatenate([stacked(g), stacked(g + 1)], axis=1)).astype(BF16)
        for i in range(2):
            out[n * (g + i) : n * (g + i + 1), :] = both[:, LANES * i : LANES * (i + 1)]


def unpack_body(parts, gate_rows, out):
    n = NX * BLOCK_ROWS
    total = parts[0:n, :].astype(F32)
    for y in range(1, NY):
        total = total + parts[n * y : n * (y + 1), :].astype(F32)
    slot = slot_of(gate_rows[...])
    place, chunk = divided(iota((TOK * HALF, 1), 0), HALF)
    place = place + NC * (FIRST_PLANE_OUT - FIRST_PLANE_IN)
    token = place - TOK * jnp.floor((place + 0.5) * (1.0 / TOK))
    spread = dot(one_hot(token, iota((TOK * HALF, TOK), 1)), slot.astype(BF16))
    key = chunk * 16.0 + spread[:, 0:1]
    out[...] = dot(one_hot(key, chunk_and_slot(iota((1, n), 1))), total.astype(BF16)).astype(BF16)


def finish_body(parts, out, total):
    n = NC * HALF
    value = parts[0:n, :].astype(F32)
    for z in range(1, NZ):
        value = value + parts[n * z : n * (z + 1), :].astype(F32)
    total[...] = value
    for j in range(n):
        out[:, j * LANES : (j + 1) * LANES] = total[j : j + 1, :].astype(BF16)


def turned(members, first):
    return [(i + first) % members for i in range(members)]


ROW_ORDER = [i ^ 2 for i in range(NC * NX)]


def exchange(x, axes, members, order, group=8):
    rows = x.shape[0] // members
    y = lax.all_to_all(
        x.reshape(members, rows // group, group, x.shape[1]),
        axes,
        split_axis=0,
        concat_axis=0,
        axis_index_groups=[order],
        tiled=True,
    )
    return y.reshape(x.shape)


def up_parts_body(place_ids, far_w, core_out, row_out, both_out, done):
    core, xh = place_ids[0], place_ids[1]
    to = (2 * (1 - core) + xh, 2 * core + 1 - xh, 2 * (1 - core) + 1 - xh)
    copies = [
        pltpu.make_async_copy(far_w.at[rows_at(eighth * WIDTH, WIDTH)], out, done.at[i])
        for i, (eighth, out) in enumerate(zip(to, (core_out, row_out, both_out)))
    ]
    for copy in copies:
        copy.start()
    for copy in copies:
        copy.wait()


def down_row_body(place_ids, w_out, other, *outs):
    core, x = place_ids[0], place_ids[2]
    for d, out in enumerate(outs):
        to = (core * NX + lax.bitwise_xor(x, jnp.int32(d))) * WIDTH
        out[0:BLOCK, :] = w_out[:, rows_at(to, WIDTH)]
        out[BLOCK : 2 * BLOCK, :] = other[:, rows_at(to, WIDTH)]


def up_weights(place_ids, w_in):
    parts = call(
        up_parts_body,
        (jax.ShapeDtypeStruct((WIDTH, 2 * LANES), BF16),) * 3,
        (place_ids, w_in),
        scratch=(pltpu.SemaphoreType.DMA((3,)),),
        smem=(0,),
        far=(1,),
    )
    swaps = ("c", [(0, 1), (1, 0)]), ("xh", [(0, 1), (1, 0)]), (("c", "xh"), [(i, 3 - i) for i in range(4)])
    out = []
    for i in (1, 2, 0):
        out.append(lax.ppermute(parts[i], *swaps[i]))
    return out[2], out[0], out[1]


def down_weights(place_ids, w_out):
    other = lax.ppermute(w_out, "c", [(0, 1), (1, 0)])
    parts = call(
        down_row_body,
        (jax.ShapeDtypeStruct((2 * BLOCK, WIDTH), BF16),) * NX,
        (place_ids, w_out, other),
        smem=(0,),
    )
    parts = list(parts)
    for d in range(1, NX):
        parts[d] = lax.ppermute(parts[d], ("xh", "xl"), [(i, i ^ d) for i in range(NX)])
    return parts


def layer(tokens, node_ids, gates, w_in, w_out):
    shape = jax.ShapeDtypeStruct
    core, xh, xl = (lax.axis_index(a).astype(jnp.int32) for a in ROW)
    place_ids = jnp.stack([core, xh, xh * NXL + xl])

    sent = call(
        spread_body,
        shape((TOK * TOKEN_ROWS, LANES), BF16),
        (node_ids[0], gates[0], tokens[0]),
        scratch=(
            pltpu.VMEM((1, 4), jnp.int32),
            pltpu.VMEM((1, 8), BF16),
            pltpu.VMEM((1, 2 * HALF * LANES), BF16),
            pltpu.VMEM((2 * NC * TOKEN_ROWS, LANES), F32),
            pltpu.SemaphoreType.DMA((3,)),
        ),
        far=(0, 1, 2),
    )
    sent, w_in, w_out = lax.optimization_barrier((sent, w_in, w_out))
    arrived = exchange(sent, COLUMN, NZ * NC, turned(NZ * NC, NC * FIRST_PLANE_IN), 2)
    w_in = w_in.reshape(4 * WIDTH, 2 * LANES)
    w_up = up_weights(place_ids, w_in)
    w_down = down_weights(place_ids, w_out[0])

    packed, gate_rows = call(
        pack_body,
        (shape((NY * NX * BLOCK_ROWS, LANES), BF16), shape((TOK, LANES), F32)),
        (arrived,),
    )
    rows = exchange(packed, PLANE, NY * NX, turned(NY * NX, FIRST_COLUMN))

    partial_sums, gate, balance = call(
        up_body,
        (shape((8 * ROWS, LANES), BF16), shape((ROWS, LANES), F32), shape((1,), F32)),
        (place_ids, w_in, rows, *w_up),
        scratch=(
            pltpu.VMEM((EIGHTH + 1, ROWS, LANES), F32),
            pltpu.VMEM((WIDTH, 2 * LANES), BF16),
            pltpu.SemaphoreType.DMA((1,)),
        ),
        smem=(0,),
        smem_out=(2,),
        far=(1,),
        flops=10**9,
    )
    summands = exchange(partial_sums, ROW, 8, ROW_ORDER)

    hidden = call(hidden_body, shape((4 * ROWS, LANES), BF16), (summands, gate))
    every_hidden = exchange(hidden, ROW, 8, ROW_ORDER)

    down = call(
        down_body,
        shape((NY * NX * BLOCK_ROWS, LANES), BF16),
        (place_ids, every_hidden, *w_down),
        scratch=(pltpu.VMEM((ROWS, WIDTH), F32),),
        smem=(0,),
        flops=10**9,
    )
    returned = exchange(down, PLANE, NY * NX, turned(NY * NX, FIRST_COLUMN))

    unpacked = call(
        unpack_body,
        shape((TOK * HALF, LANES), BF16),
        (returned, gate_rows),
    )
    back = exchange(unpacked, COLUMN, NZ * NC, turned(NZ * NC, NC * FIRST_PLANE_OUT), 4)

    mixed = call(
        finish_body,
        shape((1, 2 * HALF * LANES), BF16),
        (back,),
        scratch=(pltpu.VMEM((2 * HALF, LANES), F32),),
    )
    return mixed[None], balance


def solution(mesh):
    fine = Mesh(mesh.devices.reshape(NZ, NC, NY, NXH, NXL), AXES)
    token_spec = P(PLANE, COLUMN, None)
    return jax.shard_map(
        layer,
        mesh=fine,
        in_specs=(
            token_spec,
            token_spec,
            token_spec,
            P(AXES, None, None),
            P(COLUMN, PLANE, None),
        ),
        out_specs=(token_spec, P(COLUMN)),
        check_vma=False,
    )
```
